32 devices in a mesh: row: 16 (over z, y, core), col: 2 (over x).
Axes of the slice: x: 2, y: 2, z: 4, core: 2. Of those that a mesh axis runs over, the one named last changes fastest.
Arguments:
- tokens: bfloat16 [16384, 512], P('row', 'col'), may hold values from -6 to 6
- prev_logits: bfloat16 [16, 8, 1024, 1024], P('row', 'col'), may hold values from -9 to 9
- qkv_weight: bfloat16 [512, 1536], P('row', 'col'), may hold values from -0.25 to 0.25
- qkv_bias: bfloat16 [1536], P('col'), may hold values from -2 to 2
- out_weight: bfloat16 [512, 512], P('col', 'row'), may hold values from -1 to 1
- out_bias: bfloat16 [512], P('col'), may hold values from -1.5 to 1.5
- norm1_gain: bfloat16 [512], P('col'), may hold values from 0.25 to 1.75
- norm1_shift: bfloat16 [512], P('col'), may hold values from -2 to 2
- ff1_weight: bfloat16 [512, 2048], P('row', 'col'), may hold values from -0.25 to 0.25
- ff1_bias: bfloat16 [2048], P('col'), may hold values from -2 to 2
- ff2_weight: bfloat16 [2048, 512], P('col', 'row'), may hold values from -0.125 to 0.125
- ff2_bias: bfloat16 [512], P('col'), may hold values from -1.5 to 1.5
- norm2_gain: bfloat16 [512], P('col'), may hold values from 0.25 to 1.75
- norm2_shift: bfloat16 [512], P('col'), may hold values from -2 to 2
- out_grad: bfloat16 [16384, 512], P('row', 'col'), may hold values from -6 to 6
- logit_grad: bfloat16 [16, 8, 1024, 1024], P('row', 'col'), may hold values from -0.3984375 to 0.3984375
Outputs:
- output: bfloat16 [16384, 512], P('row', 'col')
- raw_logits: bfloat16 [16, 8, 1024, 1024], P('row', 'col')
- input_grad: bfloat16 [16384, 512], P('row', 'col')
- prev_grad: bfloat16 [16, 8, 1024, 1024], P('row', 'col')
- qkv_weight_grad: float32 [512, 1536], P('row', 'col')
- qkv_bias_grad: float32 [1536], P('col')
- out_weight_grad: float32 [512, 512], P('col', 'row')
- out_bias_grad: float32 [512], P('col')
- norm1_gain_grad: float32 [512], P('col')
- norm1_shift_grad: float32 [512], P('col')
- ff1_weight_grad: float32 [512, 2048], P('row', 'col')
- ff1_bias_grad: float32 [2048], P('col')
- ff2_weight_grad: float32 [2048, 512], P('col', 'row')
- ff2_bias_grad: float32 [512], P('col')
- norm2_gain_grad: float32 [512], P('col')
- norm2_shift_grad: float32 [512], P('col')
The draws below stay inside these ranges and needn't reach their ends.
All inputs are finite; a program needn't handle non-finite values.
Results may differ from the reference program's by a relative error of at most 0.011.
Values may be sent and summed in bfloat16 or wider, within the bound.
A program may use at most 128 MiB of HBM per device.

```python
import math
import jax
import jax.numpy as jnp
from jax import lax

D = 512
H = 8
DH = 64
FF = 2048
SEQ_LEN = 1024
TOKENS = 16384
SEQS = 16


def block_levels(own_key, shape, pieces, low, top_value):
    def one(axis_at, blocks):
        steps = jax.random.uniform(jax.random.fold_in(jax.random.fold_in(own_key, 6), axis_at), (blocks,), jnp.float32, low / len(pieces), top_value / len(pieces))
        return jnp.repeat(jnp.exp(steps), shape[axis_at] // blocks).reshape((-1,) + (1,) * (len(shape) - axis_at - 1))

    level = one(*pieces[0])
    for cut in pieces[1:]:
        level = level * one(*cut)
    return level


def gaussian(own_key, shape, scale, bound, shards=(), kind=jnp.bfloat16):
    values = scale * jax.random.normal(own_key, shape, jnp.float32)
    if shards:
        values = values * block_levels(own_key, shape, shards, -0.22, 0.18)
    return jnp.clip(values, -bound, bound).astype(kind)


def setup_inputs(seed: int = 0) -> dict:
    key_of = jax.random.split(jax.random.key(seed), 17)
    tokens = gaussian(key_of[0], (TOKENS, D), 1.0, 6.0, ((0, 16), (1, 2)))
    prev_logits = gaussian(key_of[1], (SEQS, H, SEQ_LEN, SEQ_LEN), 1.5, 9.0, ((0, 16), (1, 2)))
    qkv_weight = gaussian(key_of[2], (D, 3 * D), D ** -0.5, 0.25, ((0, 16), (1, 2)))
    qkv_bias = gaussian(key_of[3], (3 * D,), 0.3, 2.0, ((0, 2),))
    out_weight = gaussian(key_of[4], (D, D), (D // 16) ** -0.5, 1.0, ((0, 2), (1, 16)))
    out_bias = gaussian(key_of[5], (D,), 0.2, 1.5, ((0, 2),))
    norm1_gain = jnp.clip(1.0 + 0.15 * jax.random.normal(key_of[6], (D,), jnp.float32), 0.25, 1.75).astype(jnp.bfloat16)
    norm1_shift = gaussian(key_of[7], (D,), 0.3, 2.0, ((0, 2),))
    ff1_weight = gaussian(key_of[8], (D, FF), D ** -0.5, 0.25, ((0, 16), (1, 2)))
    ff1_bias = gaussian(key_of[9], (FF,), 0.3, 2.0, ((0, 2),))
    ff2_weight = gaussian(key_of[10], (FF, D), FF ** -0.5, 0.125, ((0, 2), (1, 16)))
    ff2_bias = gaussian(key_of[11], (D,), 0.2, 1.5, ((0, 2),))
    norm2_gain = jnp.clip(1.0 + 0.15 * jax.random.normal(key_of[12], (D,), jnp.float32), 0.25, 1.75).astype(jnp.bfloat16)
    norm2_shift = gaussian(key_of[13], (D,), 0.3, 2.0, ((0, 2),))
    out_grad = gaussian(key_of[14], (TOKENS, D), 1.0, 6.0, ((0, 16), (1, 2)))
    logit_grad = gaussian(key_of[15], (SEQS, H, SEQ_LEN, SEQ_LEN), 0.05, 0.3984375, ((0, 16), (1, 2)))
    return {"tokens": tokens, "prev_logits": prev_logits, "qkv_weight": qkv_weight, "qkv_bias": qkv_bias, "out_weight": out_weight, "out_bias": out_bias, "norm1_gain": norm1_gain, "norm1_shift": norm1_shift, "ff1_weight": ff1_weight, "ff1_bias": ff1_bias, "ff2_weight": ff2_weight, "ff2_bias": ff2_bias, "norm2_gain": norm2_gain, "norm2_shift": norm2_shift, "out_grad": out_grad, "logit_grad": logit_grad}


@jax.custom_vjp
def low(v):
    return lax.optimization_barrier(v.astype(jnp.bfloat16)).astype(jnp.float32)

@jax.custom_vjp
def low_back(v):
    return v

def low_keep(v):
    return (low(v), None)

def low_pass(kept, grad):
    return (grad,)

def back_keep(v):
    return (v, None)

def back_low(kept, grad):
    return (low(grad),)
low.defvjp(low_keep, low_pass)
low_back.defvjp(back_keep, back_low)
highest = lax.Precision.HIGHEST
norm_eps = 1e-06
root_half = 0.7071067811865476

def gelu_value(inner):
    return inner * 0.5 * (1.0 + lax.erf(inner * root_half))

def normalize(hidden, gain, shift):
    center = hidden - lax.optimization_barrier(jnp.mean(hidden, axis=-1, keepdims=True))
    variance = lax.optimization_barrier(jnp.mean(center * center, axis=-1, keepdims=True))
    return center * lax.rsqrt(variance + norm_eps) * gain + shift

def attend(operands):
    queries, keys_here, values_here, previous = operands
    score_scale = 1.0 / math.sqrt(DH)
    scores = low_back(previous + jnp.einsum('hqe,hke->hqk', queries, keys_here, precision=highest) * score_scale)
    top_score = lax.optimization_barrier(jnp.max(scores, axis=-1, keepdims=True))
    exponent = jnp.exp(scores - top_score)
    probs = low(exponent / lax.optimization_barrier(jnp.sum(exponent, axis=-1, keepdims=True)))
    attended = jnp.einsum('hqk,hke->hqe', probs, values_here, precision=highest)
    return (attended, low(scores))

def layer_forward(source, previous, triple_weight, triple_bias, mix_weight, mix_bias, gain_one, shift_one, expand_weight, expand_bias, reduce_weight, reduce_bias, gain_two, shift_two):
    projected = low(low_back(jnp.dot(source, triple_weight, precision=highest) + triple_bias))
    split_heads = projected.reshape(SEQS, SEQ_LEN, H, 3, DH).transpose(3, 0, 2, 1, 4)
    attended, raw_scores = lax.map(jax.checkpoint(attend), (split_heads[0], split_heads[1], split_heads[2], previous))
    merged = low(low_back(attended.transpose(0, 2, 1, 3).reshape(TOKENS, D)))
    branch_one = low_back(jnp.dot(merged, mix_weight, precision=highest) + mix_bias)
    normed_one = normalize(source + branch_one, gain_one, shift_one)
    inner = low_back(jnp.dot(low(normed_one), expand_weight, precision=highest) + expand_bias)
    activated = low(gelu_value(inner))
    branch_two = low_back(jnp.dot(activated, reduce_weight, precision=highest) + reduce_bias)
    return (normalize(normed_one + branch_two, gain_two, shift_two), raw_scores)

def reference(tokens, prev_logits, qkv_weight, qkv_bias, out_weight, out_bias, norm1_gain, norm1_shift, ff1_weight, ff1_bias, ff2_weight, ff2_bias, norm2_gain, norm2_shift, out_grad, logit_grad):
    primals = tuple((item.astype(jnp.float32) for item in (tokens, prev_logits, qkv_weight, qkv_bias, out_weight, out_bias, norm1_gain, norm1_shift, ff1_weight, ff1_bias, ff2_weight, ff2_bias, norm2_gain, norm2_shift)))
    (result, raw_scores), pullback = jax.vjp(layer_forward, *primals)
    grads = pullback((out_grad.astype(jnp.float32), logit_grad.astype(jnp.float32)))
    return (result.astype(jnp.bfloat16), raw_scores.astype(jnp.bfloat16), grads[0].astype(jnp.bfloat16), grads[1].astype(jnp.bfloat16), grads[2], grads[3], grads[4], grads[5], grads[6], grads[7], grads[8], grads[9], grads[10], grads[11], grads[12], grads[13])
```

```python
import functools
import math

import jax
import jax.numpy as jnp
from jax import lax
from jax.experimental import pallas as pl
from jax.experimental.pallas import tpu as pltpu
from jax.sharding import PartitionSpec as P

DH = 64
F32 = jnp.float32
BF16 = jnp.bfloat16
norm_eps = 1e-06
root_half = 0.7071067811865476
inv_root_two_pi = 0.3989422804014327
NT = (((1,), (1,)), ((), ()))
TN = (((0,), (0,)), ((), ()))


def dot_nn(a, b):
    return jnp.dot(a, b, preferred_element_type=F32)


def dot_nt(a, b):
    return lax.dot_general(a, b, NT, preferred_element_type=F32)


def dot_tn(a, b):
    return lax.dot_general(a, b, TN, preferred_element_type=F32)


def pick(value, index, width):
    if width == DH:
        return value
    lane = lax.broadcasted_iota(jnp.int32, value.shape, 1)
    keep = (lane >= index * DH) & (lane < (index + 1) * DH)
    return jnp.where(keep, value, jnp.zeros_like(value))


def part_of(proj, pair, heads, part):
    pieces = [
        proj[:, (pair * heads + i) * 3 * DH + part * DH :][:, :DH] for i in range(heads)
    ]
    return pieces[0] if heads == 1 else jnp.concatenate(pieces, axis=1)


def forward_block(q_rows, k_all, v_masked, prev, width):
    raws, probs, total = [], [], None
    for i in range(width // DH):
        scores = dot_nt(pick(q_rows, i, width), k_all) + prev[i].astype(F32)
        raws.append(scores.astype(BF16))
        exponent = jnp.exp(scores - jnp.max(scores, axis=1, keepdims=True))
        scale = 1.0 / jnp.sum(exponent, axis=1, keepdims=True)
        prob = (exponent * scale).astype(BF16)
        probs.append(prob)
        out = dot_nn(prob, v_masked[i])
        total = out if total is None else total + out
    return raws, probs, total


def attend_forward_kernel(heads, pairs, proj_ref, prev_ref, raw_ref, prob_ref, out_ref, q_s, k_s, v_s):
    width = heads * DH
    rows = prev_ref.shape[1]
    block = pl.program_id(1)

    @pl.when(block == 0)
    def _():
        for pair in range(pairs):

            @pl.when(lax.rem(pl.program_id(0), pairs) == pair)
            def _():
                proj = proj_ref[...]
                q_s[...] = part_of(proj, pair, heads, 0) * jnp.asarray(0.125, BF16)
                k_s[...] = part_of(proj, pair, heads, 1)
                v = part_of(proj, pair, heads, 2)
                for i in range(heads):
                    v_s[i] = pick(v, i, width)

    q_rows = q_s[pl.ds(pl.multiple_of(block * rows, rows), rows), :]
    raws, probs, out = forward_block(
        q_rows, k_s[...], [v_s[i] for i in range(heads)], [prev_ref[i] for i in range(heads)], width
    )
    for i in range(heads):
        raw_ref[i] = raws[i]
        prob_ref[i] = probs[i]
    out_ref[...] = out.astype(BF16)


def attend_forward(proj, prev, seqs, head_count, rows):
    heads = min(2, head_count)
    pairs = head_count // heads
    length = prev.shape[-1]
    width = heads * DH
    group = lambda g, b: (g, b, 0)
    return pl.pallas_call(
        functools.partial(attend_forward_kernel, heads, pairs),
        grid=(seqs * pairs, length // rows),
        in_specs=[
            pl.BlockSpec((length, proj.shape[1]), lambda g, b: (g // pairs, 0)),
            pl.BlockSpec((heads, rows, length), group),
        ],
        out_specs=[
            pl.BlockSpec((heads, rows, length), group),
            pl.BlockSpec((heads, rows, length), group),
            pl.BlockSpec((rows, width), lambda g, b: ((g // pairs) * (length // rows) + b, g % pairs)),
        ],
        out_shape=[
            jax.ShapeDtypeStruct(prev.shape, BF16),
            jax.ShapeDtypeStruct(prev.shape, BF16),
            jax.ShapeDtypeStruct((seqs * length, head_count * DH), BF16),
        ],
        scratch_shapes=[
            pltpu.VMEM((length, width), BF16),
            pltpu.VMEM((length, width), BF16),
            pltpu.VMEM((heads, length, width), BF16),
        ],
        name="attend_forward",
    )(proj, prev)


def attend_backward_kernel(
    heads, pairs, proj_ref, prob_ref, grad_ref, cot_ref, pg_ref, dproj_ref, q_s, k_s, v_s, dq_s, dk_s, dv_s
):
    width = heads * DH
    rows = prob_ref.shape[1]
    block = pl.program_id(1)
    pair_now = lax.rem(pl.program_id(0), pairs)

    @pl.when(block == 0)
    def _():
        for pair in range(pairs):

            @pl.when(pair_now == pair)
            def _():
                proj = proj_ref[...]
                q_s[...] = part_of(proj, pair, heads, 0) * jnp.asarray(0.125, BF16)
                k = part_of(proj, pair, heads, 1)
                for i in range(heads):
                    k_s[i] = pick(k, i, width)
                v_s[...] = part_of(proj, pair, heads, 2)

        dk_s[...] = jnp.zeros_like(dk_s)
        dv_s[...] = jnp.zeros_like(dv_s)

    at = pl.ds(pl.multiple_of(block * rows, rows), rows)
    q_rows = q_s[at, :]
    d_rows = grad_ref[...]
    dq = None
    dk = None
    dv = None
    for i in range(heads):
        d_one = pick(d_rows, i, width)
        d_probs = dot_nt(d_one, v_s[...])
        prob = prob_ref[i]
        wide = prob.astype(F32)
        delta = jnp.sum(d_probs * wide, axis=1, keepdims=True)
        low = (wide * (d_probs - delta) + cot_ref[i].astype(F32)).astype(BF16)
        pg_ref[i] = low
        a = dot_nn(low, k_s[i])
        b = dot_tn(pick(q_rows, i, width), low)
        c = dot_tn(d_one, prob)
        dq = a if dq is None else dq + a
        dk = b if dk is None else dk + b
        dv = c if dv is None else dv + c
    dq_s[at, :] = (dq * 0.125).astype(BF16)
    dk_s[...] += dk
    dv_s[...] += dv

    @pl.when(block == pl.num_programs(1) - 1)
    def _():
        for pair in range(pairs):

            @pl.when(pair_now == pair)
            def _():
                parts = [dq_s[...], dk_s[...].T.astype(BF16), dv_s[...].T.astype(BF16)]
                for i in range(heads):
                    base = (pair * heads + i) * 3 * DH
                    dproj_ref[:, base : base + 3 * DH] = jnp.concatenate(
                        [p[:, i * DH : (i + 1) * DH] for p in parts], axis=1
                    )


def attend_backward(proj, prob, grad, cot, seqs, head_count, rows):
    heads = min(2, head_count)
    pairs = head_count // heads
    length = prob.shape[-1]
    width = heads * DH
    group = lambda g, b: (g, b, 0)
    return pl.pallas_call(
        functools.partial(attend_backward_kernel, heads, pairs),
        grid=(seqs * pairs, length // rows),
        in_specs=[
            pl.BlockSpec((length, proj.shape[1]), lambda g, b: (g // pairs, 0)),
            pl.BlockSpec((heads, rows, length), group),
            pl.BlockSpec((rows, width), lambda g, b: ((g // pairs) * (length // rows) + b, g % pairs)),
            pl.BlockSpec((heads, rows, length), group),
        ],
        out_specs=[
            pl.BlockSpec((heads, rows, length), group),
            pl.BlockSpec((length, proj.shape[1]), lambda g, b: (g // pairs, 0)),
        ],
        out_shape=[
            jax.ShapeDtypeStruct(prob.shape, BF16),
            jax.ShapeDtypeStruct(proj.shape, BF16),
        ],
        scratch_shapes=[
            pltpu.VMEM((length, width), BF16),
            pltpu.VMEM((heads, length, width), BF16),
            pltpu.VMEM((length, width), BF16),
            pltpu.VMEM((length, width), BF16),
            pltpu.VMEM((width, length), F32),
            pltpu.VMEM((width, length), F32),
        ],
        name="attend_backward",
    )(proj, prob, grad, cot)


def normalize(hidden):
    width = hidden.shape[1]
    center = hidden - jnp.sum(hidden, axis=1, keepdims=True) * (1.0 / width)
    inv_std = lax.rsqrt(jnp.sum(center * center, axis=1, keepdims=True) * (1.0 / width) + norm_eps)
    return center * inv_std, inv_std


def norm_back(scaled, xhat, inv_std):
    width = scaled.shape[1]
    mean_grad = jnp.sum(scaled, axis=1, keepdims=True) * (1.0 / width)
    mean_cross = jnp.sum(scaled * xhat, axis=1, keepdims=True) * (1.0 / width)
    return inv_std * (scaled - mean_grad - xhat * mean_cross)


def col_sum(value):
    return jnp.sum(value, axis=0, keepdims=True)


def middle_kernel(
    tok_ref, att_ref, og_ref, w_ref, vec_ref, ffb_ref, out_ref, dh_ref, datt_ref, gw_ref, gvec_ref, gffb_ref, act_s, slope_s
):
    cols = w_ref.shape[0]
    width = vec_ref.shape[1]
    hw = width // cols
    fw = ffb_ref.shape[1] // cols
    cut = min(512, fw)
    att = [att_ref[:, c * hw : (c + 1) * hw] for c in range(cols)]
    vec = vec_ref[...].astype(F32)
    out_bias, gain1, shift1, ff2_bias, gain2, shift2 = (vec[i : i + 1] for i in range(6))

    branch = None
    for c in range(cols):
        t = dot_nt(att[c], w_ref[c, :, :hw])
        branch = t if branch is None else branch + t
    hidden1 = tok_ref[...].astype(F32) + branch + out_bias
    xhat1, inv1 = normalize(hidden1)
    normed1 = xhat1 * gain1 + shift1
    low1 = normed1.astype(BF16)

    chunks = [(c, o) for c in range(cols) for o in range(0, fw, cut)]
    hidden2 = normed1 + ff2_bias
    for c, o in chunks:
        at = c * fw + o
        inner = dot_nn(low1, w_ref[c, :, hw + o : hw + o + cut]) + ffb_ref[:, at : at + cut].astype(F32)
        half = 0.5 + 0.5 * lax.erf(inner * root_half)
        act = (inner * half).astype(BF16)
        act_s[:, at : at + cut] = act
        slope_s[:, at : at + cut] = half + inner * inv_root_two_pi * jnp.exp(-0.5 * inner * inner)
        hidden2 = hidden2 + dot_nt(act, w_ref[c, :, hw + fw + o : hw + fw + o + cut])
    xhat2, inv2 = normalize(hidden2)
    out_ref[...] = (xhat2 * gain2 + shift2).astype(BF16)

    og = og_ref[...].astype(F32)
    d_hidden2 = norm_back(og * gain2, xhat2, inv2)
    low2 = d_hidden2.astype(BF16)
    rows = [None] * 6
    rows[4] = col_sum(og * xhat2)
    rows[5] = col_sum(og)
    rows[3] = col_sum(low2.astype(F32))
    low1_t = low1.T
    low2_t = low2.T
    d_normed1 = d_hidden2
    for c, o in chunks:
        at = c * fw + o
        d_act = dot_nn(low2, w_ref[c, :, hw + fw + o : hw + fw + o + cut])
        d_inner = (d_act * slope_s[:, at : at + cut]).astype(BF16)
        d_normed1 = d_normed1 + dot_nt(d_inner, w_ref[c, :, hw + o : hw + o + cut])
        gw_ref[c, :, hw + o : hw + o + cut] = dot_nn(low1_t, d_inner).astype(BF16)
        gw_ref[c, :, hw + fw + o : hw + fw + o + cut] = dot_nn(low2_t, act_s[:, at : at + cut]).astype(BF16)
        gffb_ref[:, at : at + cut] = col_sum(d_inner.astype(F32))

    rows[1] = col_sum(d_normed1 * xhat1)
    rows[2] = col_sum(d_normed1)
    d_hidden1 = norm_back(d_normed1 * gain1, xhat1, inv1)
    dh_ref[...] = d_hidden1.astype(dh_ref.dtype)
    low = d_hidden1.astype(BF16)
    rows[0] = col_sum(low.astype(F32))
    low_t = low.T
    for c in range(cols):
        datt_ref[:, c * hw : (c + 1) * hw] = dot_nn(low, w_ref[c, :, :hw]).astype(BF16)
        gw_ref[c, :, :hw] = dot_nn(low_t, att[c]).astype(BF16)
    gvec_ref[...] = jnp.concatenate(rows, axis=0)


def middle(tok, att, og, w, vec, ffb):
    rows, width = tok.shape
    hidden = ffb.shape[1]
    return pl.pallas_call(
        middle_kernel,
        out_shape=[
            jax.ShapeDtypeStruct((rows, width), BF16),
            jax.ShapeDtypeStruct((rows, width), F32),
            jax.ShapeDtypeStruct((rows, width), BF16),
            jax.ShapeDtypeStruct(w.shape, BF16),
            jax.ShapeDtypeStruct((6, width), F32),
            jax.ShapeDtypeStruct((1, hidden), F32),
        ],
        in_specs=[pl.BlockSpec(memory_space=pltpu.VMEM)] * 6,
        out_specs=[pl.BlockSpec(memory_space=pltpu.VMEM)] * 6,
        scratch_shapes=[pltpu.VMEM((rows, hidden), BF16), pltpu.VMEM((rows, hidden), F32)],
        compiler_params=pltpu.CompilerParams(vmem_limit_bytes=60 << 20),
        name="middle",
    )(tok, att, og, w, vec, ffb)


def per_device(
    cols,
    tokens,
    prev_logits,
    qkv_weight,
    qkv_bias,
    out_weight,
    out_bias,
    norm1_gain,
    norm1_shift,
    ff1_weight,
    ff1_bias,
    ff2_weight,
    ff2_bias,
    norm2_gain,
    norm2_shift,
    out_grad,
    logit_grad,
):
    seqs, head_count, length, _ = prev_logits.shape
    total, feat = tokens.shape
    share = total // cols
    rows = min(256, length)
    me = lax.axis_index("col")

    def to_rows(x):
        return lax.all_to_all(x, "col", split_axis=0, concat_axis=1, tiled=True)

    def to_features(x):
        return lax.all_to_all(x, "col", split_axis=1, concat_axis=0, tiled=True)

    tokens_full = lax.all_gather(tokens, "col", axis=1, tiled=True)
    wide_qkv = lax.all_gather(qkv_weight, "row", axis=0, tiled=True)
    mixed = jnp.concatenate([out_weight.T, ff1_weight, ff2_weight.T], axis=1)
    mixed = lax.all_gather(lax.all_gather(mixed, "row", axis=0, tiled=True), "col", axis=0)
    vectors = jnp.stack([out_bias, norm1_gain, norm1_shift, ff2_bias, norm2_gain, norm2_shift])
    vectors = lax.all_gather(vectors, "col", axis=1, tiled=True)
    ff1_bias_full = lax.all_gather(ff1_bias, "col", axis=0, tiled=True)[None]
    og = to_rows(out_grad)

    proj = (dot_nn(tokens_full, wide_qkv) + qkv_bias.astype(F32)).astype(BF16)
    prev = prev_logits.reshape(seqs * head_count, length, length)
    cot = logit_grad.reshape(seqs * head_count, length, length)
    raw, prob, att = attend_forward(proj, prev, seqs, head_count, rows)
    att_rows = to_rows(att)
    tok_rows = lax.dynamic_slice_in_dim(tokens_full, me * share, share, 0)
    out, dh, datt, gw, gvec, gffb = middle(tok_rows, att_rows, og, mixed, vectors, ff1_bias_full)
    output = to_features(out)
    d_hidden = to_features(dh)
    datt_full = to_features(datt)
    prev_grad, dproj = attend_backward(proj, prob, datt_full, cot, seqs, head_count, rows)

    input_part = lax.psum_scatter(
        dot_nt(dproj, wide_qkv), "col", scatter_dimension=1, tiled=True
    )
    input_grad = (d_hidden + input_part).astype(BF16)
    qkv_grad = lax.psum_scatter(dot_tn(tokens_full, dproj), "row", scatter_dimension=0, tiled=True)
    qkv_bias_grad = jnp.sum(dproj.astype(F32), axis=0)
    gw = lax.psum_scatter(gw.astype(F32), "row", scatter_dimension=1, tiled=True)
    gw = lax.psum_scatter(gw, "col", scatter_dimension=0, tiled=True)[0]
    hidden = ff1_weight.shape[1]
    vec_sum = lax.psum_scatter(
        jnp.concatenate(
            [gvec.reshape(6, cols, feat).transpose(1, 0, 2).reshape(cols, 6 * feat), gffb.reshape(cols, hidden)],
            axis=1,
        ),
        "col",
        scatter_dimension=0,
        tiled=True,
    )[0]
    vec_sum, qkv_bias_grad = lax.psum((vec_sum, qkv_bias_grad), "row")
    vs = [vec_sum[i * feat : (i + 1) * feat] for i in range(6)]
    return (
        output,
        raw.reshape(prev_logits.shape),
        input_grad,
        prev_grad.reshape(prev_logits.shape),
        qkv_grad,
        qkv_bias_grad,
        gw[:, :feat].T,
        vs[0],
        vs[1],
        vs[2],
        gw[:, feat : feat + hidden],
        vec_sum[6 * feat :],
        gw[:, feat + hidden :].T,
        vs[3],
        vs[4],
        vs[5],
    )


def solution(mesh):
    in_specs = (
        P("row", "col"),
        P("row", "col", None, None),
        P("row", "col"),
        P("col"),
        P("col", "row"),
        P("col"),
        P("col"),
        P("col"),
        P("row", "col"),
        P("col"),
        P("col", "row"),
        P("col"),
        P("col"),
        P("col"),
        P("row", "col"),
        P("row", "col", None, None),
    )
    out_specs = (
        P("row", "col"),
        P("row", "col", None, None),
        P("row", "col"),
        P("row", "col", None, None),
        P("row", "col"),
        P("col"),
        P("col", "row"),
        P("col"),
        P("col"),
        P("col"),
        P("row", "col"),
        P("col"),
        P("col", "row"),
        P("col"),
        P("col"),
        P("col"),
    )
    return jax.shard_map(
        functools.partial(per_device, mesh.shape["col"]),
        mesh=mesh,
        in_specs=in_specs,
        out_specs=out_specs,
        check_vma=False,
    )
```

```python
import functools
import math

import jax
import jax.numpy as jnp
from jax import lax
from jax.experimental import pallas as pl
from jax.experimental.pallas import tpu as pltpu
from jax.sharding import PartitionSpec as P

DH = 64
F32 = jnp.float32
BF16 = jnp.bfloat16
norm_eps = 1e-06
root_half = 0.7071067811865476
inv_root_two_pi = 0.3989422804014327
NT = (((1,), (1,)), ((), ()))
TN = (((0,), (0,)), ((), ()))


def dot_nn(a, b):
    return jnp.dot(a, b, preferred_element_type=F32)


def dot_nt(a, b):
    return lax.dot_general(a, b, NT, preferred_element_type=F32)


def dot_tn(a, b):
    return lax.dot_general(a, b, TN, preferred_element_type=F32)


def pick(value, index, width):
    if width == DH:
        return value
    lane = lax.broadcasted_iota(jnp.int32, value.shape, 1)
    keep = (lane >= index * DH) & (lane < (index + 1) * DH)
    return jnp.where(keep, value, jnp.zeros_like(value))


def part_of(proj, pair, heads, part):
    pieces = [
        proj[:, (pair * heads + i) * 3 * DH + part * DH :][:, :DH] for i in range(heads)
    ]
    return pieces[0] if heads == 1 else jnp.concatenate(pieces, axis=1)


def forward_block(q_rows, k_all, v_masked, prev, width):
    raws, probs, total = [], [], None
    for i in range(width // DH):
        scores = dot_nt(pick(q_rows, i, width), k_all) + prev[i].astype(F32)
        raws.append(scores.astype(BF16))
        exponent = jnp.exp(scores - jnp.max(scores, axis=1, keepdims=True))
        scale = 1.0 / jnp.sum(exponent, axis=1, keepdims=True)
        prob = (exponent * scale).astype(BF16)
        probs.append(prob)
        out = dot_nn(prob, v_masked[i])
        total = out if total is None else total + out
    return raws, probs, total


def normalize(hidden):
    width = hidden.shape[1]
    center = hidden - jnp.sum(hidden, axis=1, keepdims=True) * (1.0 / width)
    inv_std = lax.rsqrt(jnp.sum(center * center, axis=1, keepdims=True) * (1.0 / width) + norm_eps)
    return center * inv_std, inv_std


def norm_back(scaled, xhat, inv_std):
    width = scaled.shape[1]
    mean_grad = jnp.sum(scaled, axis=1, keepdims=True) * (1.0 / width)
    mean_cross = jnp.sum(scaled * xhat, axis=1, keepdims=True) * (1.0 / width)
    return inv_std * (scaled - mean_grad - xhat * mean_cross)


def col_sum(value):
    return jnp.sum(value, axis=0, keepdims=True)


def middle_kernel(
    dims, tok_ref, att_ref, og_ref, w_ref, vec_ref, raw_in,
    out_ref, dh_ref, datt_ref, gw_ref, gvec_ref, raw_out,
    act_s, slope_s, bounce, in_sem, out_sem,
):
    cols, share, hw, fw = dims
    feat = vec_ref.shape[2]
    pairs, width = att_ref.shape[1], att_ref.shape[3]
    slots, rows_dev = bounce.shape[0], w_ref.shape[0]
    shard = w_ref.shape[2]
    cut = min(512, fw)
    me = lax.axis_index("col")

    takes = [pltpu.make_async_copy(raw_in.at[n], bounce.at[n], in_sem.at[n]) for n in range(slots)]
    puts = [pltpu.make_async_copy(bounce.at[n], raw_out.at[n], out_sem.at[n]) for n in range(slots)]
    for c in takes:
        c.start()

    def side(ref, i):
        return jnp.concatenate([ref[c, i : i + 1] for c in range(cols)], axis=1).astype(F32)

    def weight(c, a, b):
        return w_ref[:, c, :, a:b].reshape(rows_dev * shard, b - a)

    def put_weight(c, a, b, value):
        gw_ref[:, c, :, a:b] = value.astype(BF16).reshape(rows_dev, shard, b - a)

    own = pl.ds(pl.multiple_of(me * share, share), share)
    out_bias, gain1, shift1, ff2_bias, gain2, shift2 = (side(vec_ref, i) for i in range(6))
    tok = jnp.concatenate([tok_ref[c, own, :] for c in range(cols)], axis=1)

    hidden1 = tok.astype(F32) + out_bias
    for c in range(cols):
        for j in range(pairs):
            hidden1 = hidden1 + dot_nt(att_ref[c, j], weight(c, j * width, (j + 1) * width))
    xhat1, inv1 = normalize(hidden1)
    normed1 = xhat1 * gain1 + shift1
    low1 = normed1.astype(BF16)

    chunks = [(c, o) for c in range(cols) for o in range(0, fw, cut)]
    hidden2 = normed1 + ff2_bias
    for c, o in chunks:
        at = c * fw + o
        bias = jnp.concatenate([vec_ref[c, 6 + (o + i) // feat : 7 + (o + i) // feat] for i in range(0, cut, feat)], axis=1)
        inner = dot_nn(low1, weight(c, hw + o, hw + o + cut)) + bias.astype(F32)
        half = 0.5 + 0.5 * lax.erf(inner * root_half)
        act = (inner * half).astype(BF16)
        act_s[:, at : at + cut] = act
        slope_s[:, at : at + cut] = half + inner * inv_root_two_pi * jnp.exp(-0.5 * inner * inner)
        hidden2 = hidden2 + dot_nt(act, weight(c, hw + fw + o, hw + fw + o + cut))
    for n in range(slots):
        takes[n].wait()
        puts[n].start()
    xhat2, inv2 = normalize(hidden2)
    output = (xhat2 * gain2 + shift2).astype(BF16)

    og = jnp.concatenate([og_ref[c] for c in range(cols)], axis=1).astype(F32)
    d_hidden2 = norm_back(og * gain2, xhat2, inv2)
    low2 = d_hidden2.astype(BF16)
    rows = [None] * 6
    rows[4] = col_sum(og * xhat2)
    rows[5] = col_sum(og)
    rows[3] = col_sum(low2.astype(F32))
    low1_t = low1.T
    low2_t = low2.T
    d_normed1 = d_hidden2
    for c, o in chunks:
        at = c * fw + o
        d_act = dot_nn(low2, weight(c, hw + fw + o, hw + fw + o + cut))
        d_inner = (d_act * slope_s[:, at : at + cut]).astype(BF16)
        d_normed1 = d_normed1 + dot_nt(d_inner, weight(c, hw + o, hw + o + cut))
        put_weight(c, hw + o, hw + o + cut, dot_nn(low1_t, d_inner))
        put_weight(c, hw + fw + o, hw + fw + o + cut, dot_nn(low2_t, act_s[:, at : at + cut]))
        sums = col_sum(d_inner.astype(F32))
        for i in range(0, cut, feat):
            gvec_ref[c, 6 + (o + i) // feat : 7 + (o + i) // feat] = sums[:, i : i + feat]

    rows[1] = col_sum(d_normed1 * xhat1)
    rows[2] = col_sum(d_normed1)
    d_hidden1 = norm_back(d_normed1 * gain1, xhat1, inv1)
    low = d_hidden1.astype(BF16)
    rows[0] = col_sum(low.astype(F32))
    low_t = low.T
    spare = gvec_ref.shape[1] - 6 - fw // feat
    for c in range(cols):
        for j in range(pairs):
            put_weight(c, j * width, (j + 1) * width, dot_nn(low_t, att_ref[c, j]))
        datt_ref[c] = dot_nn(low, weight(c, 0, hw)).astype(BF16)
        span = slice(c * feat, (c + 1) * feat)
        out_ref[c] = output[:, span]
        dh_ref[c] = low[:, span]
        for i in range(6):
            gvec_ref[c, i : i + 1] = rows[i][:, span]
        if spare:
            gvec_ref[c, 6 + fw // feat :] = jnp.zeros((spare, feat), F32)
    for c in puts:
        c.wait()


def middle(tok, att, og, w, vec, raw):
    rows_dev, cols, shard, _ = w.shape
    feat = tok.shape[2]
    share = og.shape[1]
    hw = att.shape[1] * att.shape[3]
    fw = (w.shape[3] - hw) // 2
    slots = 8
    pieces = (slots, raw.shape[0] * raw.shape[1] // slots, raw.shape[2])
    vmem = pl.BlockSpec(memory_space=pltpu.VMEM)
    anywhere = pl.BlockSpec(memory_space=pl.ANY)
    results = pl.pallas_call(
        functools.partial(middle_kernel, (cols, share, hw, fw)),
        out_shape=[
            jax.ShapeDtypeStruct((cols, share, feat), BF16),
            jax.ShapeDtypeStruct((cols, share, feat), BF16),
            jax.ShapeDtypeStruct((cols, share, hw), BF16),
            jax.ShapeDtypeStruct(w.shape, BF16),
            jax.ShapeDtypeStruct(vec.shape, F32),
            jax.ShapeDtypeStruct(pieces, BF16),
        ],
        in_specs=[vmem] * 5 + [anywhere],
        out_specs=[vmem] * 5 + [anywhere],
        scratch_shapes=[
            pltpu.VMEM((share, cols * fw), BF16),
            pltpu.VMEM((share, cols * fw), F32),
            pltpu.VMEM(pieces, BF16),
            pltpu.SemaphoreType.DMA((slots,)),
            pltpu.SemaphoreType.DMA((slots,)),
        ],
        compiler_params=pltpu.CompilerParams(vmem_limit_bytes=60 << 20),
        name="middle",
    )(tok, att, og, w, vec, raw.reshape(pieces))
    return *results[:-1], results[-1].reshape(raw.shape)


MESH = pl.DeviceIdType.MESH


def chip_at(place, chips):
    place = lax.rem(place + 2 * chips, chips)
    return jnp.where(place < chips // 2, 2 * place, 2 * (chips - 1 - place) + 1)


def place_of(chip, chips):
    return jnp.where(lax.rem(chip, 2) == 0, chip // 2, chips - 1 - chip // 2)


class Spot:
    def __init__(self, devices_row, cols):
        self.cols = cols
        self.chips = devices_row // 2
        self.row = lax.axis_index("row")
        self.me = lax.axis_index("col")
        self.core = lax.rem(self.row, 2)
        self.place = place_of(self.row // 2, self.chips)
        self.partner = (self.row + 1 - 2 * self.core, self.me)

    def row_at(self, offset):
        return 2 * chip_at(self.place + offset, self.chips) + self.core

    def ring(self, way):
        return (self.row_at(1 if way == 0 else -1), self.me)

    def peer(self, j):
        return lax.rem(self.me + j + self.cols, self.cols)

    def col_peer(self, j):
        return (self.row, self.peer(j))


def greet(others):
    barrier = pltpu.get_barrier_semaphore()
    for other in others:
        pl.semaphore_signal(barrier, inc=1, device_id=other, device_id_type=MESH)
    pl.semaphore_wait(barrier, len(others))


def rcopy(src, dst, send, recv, to):
    return pltpu.make_async_remote_copy(
        src_ref=src, dst_ref=dst, send_sem=send, recv_sem=recv, device_id=to, device_id_type=MESH
    )


def cuts(weights):
    n = 2 if weights % 256 == 0 else 1
    return [pl.ds(i * (weights // n), weights // n) for i in range(n)]


def depth(chips, k, way):
    return chips // 2 if k == way else chips // 2 - 1


def front_kernel(
    dims, tok, wq, w_out, w_ff1, w_ff2, side0, side1, side2, side3, side4, side5, side6, og, bias, prev, raw, prob, tok_all, proj_all, wf_all, wq_all, vec_all, og_all, att_all,
    tok_s, wq_s, proj_s, q_s, k_s, v_s, att_s, wf, vec, wf_v,
    x_send, x_recv, q_send, q_recv, f_send, f_recv, p_send, p_recv, a_send, a_recv, l_sem,
):
    cols, rows_dev, seqs, heads, pairs, share, block = dims
    at = Spot(rows_dev, cols)
    chips, me, row = at.chips, at.me, at.row
    half_size = cols // 2
    width = heads * DH
    length = prev.shape[2]
    per = length // share
    turns = length // block
    in_share = share // block
    step = pl.program_id(0)
    steps = pairs * seqs * turns
    group = step // turns
    pos = lax.rem(step, turns)
    pair_now = group // seqs
    seq_now = lax.rem(group, seqs)
    turn = lax.rem(pos + lax.rem(me + 1, per) * in_share, turns)
    offs = [j for j in range(1, cols)]
    far = chips // 2
    pieces = cuts(wf.shape[1])
    kinds = ("tok", "tok2", "wf", "vec", "og")
    first = pl.ds(0, tok.shape[0] // 2)
    second = pl.ds(tok.shape[0] // 2, tok.shape[0] // 2)

    def half(k):
        mine = me // half_size
        first = mine if k == 0 else 1 - mine
        return pl.ds(first * half_size, half_size)

    def off(way, h):
        return -h if way == 0 else h

    def q_hop(way, h):
        r = at.row_at(off(way, h - 1))
        src = wq if h == 1 else wq_s.at[r]
        return rcopy(src, wq_s.at[r], q_send.at[way, h - 1], q_recv.at[way, h - 1], at.ring(way))

    def q_got(way, h):
        r = at.row_at(off(way, h))
        return rcopy(wq, wq_s.at[r], q_send.at[way, h - 1], q_recv.at[way, h - 1], at.ring(way))

    def q_pair(way, h, mine=True):
        r = at.row_at(off(way, h))
        src = wq if h == 0 else wq_s.at[r]
        if not mine:
            r = r + 1 - 2 * at.core
        return rcopy(src, wq_s.at[r], q_send.at[2 + way, h], q_recv.at[2 + way, h], at.partner)

    def f_hop(k, p, way, h):
        part = wf_v.at[at.row_at(off(way, h - 1)), half(k), :, pieces[p]]
        return rcopy(part, part, f_send.at[k, p, way, h - 1], f_recv.at[k, p, way, h - 1], at.ring(way))

    def f_got(k, p, way, h):
        part = wf_v.at[at.row_at(off(way, h)), half(k), :, pieces[p]]
        return rcopy(part, part, f_send.at[k, p, way, h - 1], f_recv.at[k, p, way, h - 1], at.ring(way))

    def f_pair(k, p, way, h, mine=True):
        r = at.row_at(off(way, h))
        if not mine:
            r = r + 1 - 2 * at.core
        part = wf_v.at[r, half(k), :, pieces[p]]
        return rcopy(part, part, p_send.at[k, p, way, h], p_recv.at[k, p, way, h], at.partner)

    def f_own(k, p):
        f_hop(k, p, 0, 1).start()
        f_hop(k, p, 1, 1).start()
        f_pair(k, p, 0, 0).start()

    def x_copy(kind, j):
        to = at.peer(j)
        src, dst = {
            "tok": (tok.at[first], tok_s.at[me, first]),
            "tok2": (tok.at[second], tok_s.at[me, second]),
            "wf": (wf, wf_v.at[row, me]),
            "vec": (vec, vec_all.at[me]),
            "og": (og.at[pl.ds(pl.multiple_of(to * share, share), share)], og_all.at[me]),
        }[kind]
        n = kinds.index(kind)
        return rcopy(src, dst, x_send.at[n, j - 1], x_recv.at[n, j - 1], at.col_peer(j))

    def x_got(kind, j):
        came = at.peer(-j)
        src, dst = {
            "tok": (tok.at[first], tok_s.at[came, first]),
            "tok2": (tok.at[second], tok_s.at[came, second]),
            "wf": (wf, wf_v.at[row, came]),
            "vec": (vec, vec_all.at[came]),
            "og": (og.at[pl.ds(0, share)], og_all.at[came]),
        }[kind]
        n = kinds.index(kind)
        return rcopy(src, dst, x_send.at[n, j - 1], x_recv.at[n, j - 1], at.col_peer(j))

    def locals_():
        own = pl.ds(pl.multiple_of(me * share, share), share)
        return [
            pltpu.make_async_copy(wf, wf_v.at[row, me], l_sem.at[0]),
            pltpu.make_async_copy(wq, wq_s.at[row], l_sem.at[1]),
            pltpu.make_async_copy(tok, tok_s.at[me], l_sem.at[2]),
            pltpu.make_async_copy(vec, vec_all.at[me], l_sem.at[3]),
            pltpu.make_async_copy(og.at[own], og_all.at[me], l_sem.at[4]),
        ]

    def saves():
        return [
            pltpu.make_async_copy(tok_s, tok_all, l_sem.at[0]),
            pltpu.make_async_copy(wq_s, wq_all, l_sem.at[1]),
            pltpu.make_async_copy(proj_s, proj_all, l_sem.at[2]),
        ]

    def handle(k, h, only=None):
        for p in range(len(pieces)) if only is None else only:
            for way in range(2):
                if h <= depth(chips, k, way):
                    f_got(k, p, way, h).wait_recv()
                    if h < depth(chips, k, way):
                        f_hop(k, p, way, h + 1).start()
                    f_pair(k, p, way, h).start()

    @pl.when(step == 0)
    def _():
        hw, fw = w_out.shape[1], w_ff1.shape[1]
        wf[:, :hw] = w_out[...]
        wf[:, hw : hw + fw] = w_ff1[...]
        wf[:, hw + fw :] = w_ff2[...]
        feat = vec.shape[1]
        vec[...] = jnp.zeros_like(vec)
        for i, ref in enumerate((side0, side1, side2, side3, side4, side5)):
            vec[i : i + 1, :] = ref[...].reshape(1, feat)
        long = side6[...].reshape(1, fw)
        for i in range(fw // feat):
            vec[6 + i : 7 + i, :] = long[:, i * feat : (i + 1) * feat]
        greet([at.ring(0), at.ring(1), at.partner] + [at.col_peer(j) for j in offs])
        q_hop(0, 1).start()
        q_hop(1, 1).start()
        for kind in ("wf", "tok", "tok2", "vec"):
            for j in offs:
                x_copy(kind, j).start()
        q_pair(0, 0).start()
        for c in locals_():
            c.start()
        for c in locals_():
            c.wait()
        if cols > 2:
            for j in offs:
                x_got("wf", j).wait_recv()
        for h in range(1, far + 1):
            for way in range(2):
                if h <= depth(chips, 0, way):
                    q_got(way, h).wait_recv()
                    if h < depth(chips, 0, way):
                        q_hop(way, h + 1).start()
                    q_pair(way, h).start()
            if h == 1:
                for p in range(len(pieces)):
                    f_own(0, p)
            if h == 2:
                if cols == 2:
                    for j in offs:
                        x_got("wf", j).wait_recv()
                for p in range(len(pieces)):
                    f_own(1, p)
            if h == 3:
                handle(0, 1)
        for j in offs:
            x_copy("og", j).start()
        handle(1, 1)
        for way in range(2):
            for h in range(0 if way == 0 else 1, depth(chips, 0, way) + 1):
                q_pair(way, h, mine=False).wait_recv()
        for j in offs:
            x_got("tok", j).wait_recv()
        rows = wq_s.shape[0] // cols
        chunk = min(512, tok.shape[0])

        def project(i, carry):
            span = pl.ds(pl.multiple_of(i * chunk, chunk), chunk)

            @pl.when(i == tok.shape[0] // chunk // 2)
            def _():
                for j in offs:
                    x_got("tok2", j).wait_recv()
                handle(0, 2)

            total = bias[...].reshape(1, -1).astype(F32)
            for c in range(cols):
                w = wq_s[c * rows : (c + 1) * rows].reshape(-1, wq_s.shape[2])
                total = total + dot_nn(tok_s[c, span, :], w)
            proj_s[span, :] = total.astype(BF16)
            return carry

        lax.fori_loop(0, tok.shape[0] // chunk, project, 0)
        handle(1, 2)

    @pl.when(pos == 0)
    def _():
        for pair in range(pairs):

            @pl.when(pair_now == pair)
            def _():
                proj = proj_s[pl.ds(pl.multiple_of(seq_now * length, length), length), :]
                q_s[...] = part_of(proj, pair, heads, 0) * jnp.asarray(0.125, BF16)
                k_s[...] = part_of(proj, pair, heads, 1)
                v = part_of(proj, pair, heads, 2)
                for i in range(heads):
                    v_s[i] = pick(v, i, width)

    def att_copy(g, t, to):
        i = lax.rem(me + 1 + t, per)
        j = g // seqs
        return rcopy(
            att_s.at[g, pl.ds(pl.multiple_of(i * share, share), share)],
            att_all.at[me, j],
            a_send.at[g, t],
            a_recv.at[j, me],
            (row, to),
        )

    def att_keep(g, t):
        i = lax.rem(me + 1 + t, per)
        return pltpu.make_async_copy(
            att_s.at[g, pl.ds(pl.multiple_of(i * share, share), share)], att_all.at[me, g // seqs], l_sem.at[3]
        )

    def att_to(g, t):
        return lax.rem(g, seqs) * per + lax.rem(me + 1 + t, per)

    def att_send(done):
        g = done // turns
        t = lax.rem(done, turns) // in_share
        to = att_to(g, t)

        @pl.when(to != me)
        def _():
            att_copy(g, t, to).start()

        @pl.when(to == me)
        def _():
            c = att_keep(g, t)
            c.start()
            c.wait()

    @pl.when((step > 0) & (lax.rem(step, in_share) == 0))
    def _():
        att_send(step - 1)

    at_step = {1: [(0, 3)], 2: [(1, 3)], 3: [(0, 4)], 5: [(1, 4)], 7: []}
    for h in range(5, far + 1):
        at_step[7] += [(0, h), (1, h)]
    for n, todo in at_step.items():

        @pl.when(step == n * steps // 8)
        def _(todo=todo):
            for k, h in todo:
                handle(k, h)

    @pl.when(step == 1)
    def _():
        for c in saves():
            c.start()

    rows_now = pl.ds(pl.multiple_of(turn * block, block), block)
    raws, probs, out = forward_block(
        q_s[rows_now, :], k_s[...], [v_s[i] for i in range(heads)], [prev[i] for i in range(heads)], width
    )
    for i in range(heads):
        raw[i] = raws[i]
        prob[i] = probs[i]
    att_s[group, rows_now, :] = out.astype(BF16)

    @pl.when(step == steps - 1)
    def _():
        att_send(step)
        for c in saves():
            c.wait()
        for j in offs:
            for kind in kinds:
                x_copy(kind, j).wait_send()
                if kind in ("vec", "og"):
                    x_got(kind, j).wait_recv()
        for way in range(2):
            for h in range(1, depth(chips, 0, way) + 1):
                q_hop(way, h).wait_send()
            for h in range(0 if way == 0 else 1, depth(chips, 0, way) + 1):
                q_pair(way, h).wait_send()
            for k in range(2):
                for p in range(len(pieces)):
                    for h in range(1, depth(chips, k, way) + 1):
                        f_hop(k, p, way, h).wait_send()
                    for h in range(0 if way == 0 else 1, depth(chips, k, way) + 1):
                        f_pair(k, p, way, h).wait_send()
                        f_pair(k, p, way, h, mine=False).wait_recv()
        keep = pltpu.make_async_copy(wf_v, wf_all, l_sem.at[4])
        keep.start()
        for g in range(pairs * seqs):
            for t in range(per):
                to = att_to(g, t)

                @pl.when(to != me)
                def _():
                    att_copy(g, t, to).wait_send()

        for p in range(pairs):
            for j in offs:
                came = at.peer(j)
                rcopy(
                    att_s.at[0, pl.ds(0, share)], att_all.at[came, p], a_send.at[0, 0], a_recv.at[p, came], at.col_peer(j)
                ).wait_recv()
        keep.wait()


def front(cols, rows_dev, seqs, head_count, tok, wq, w_out, w_ff1, w_ff2, sides, og, bias, prev):
    heads = min(2, head_count)
    pairs = head_count // heads
    total, feat = tok.shape
    share = total // cols
    length = prev.shape[-1]
    width = heads * DH
    block = min(256, share)
    turns = length // block
    per = length // share
    in_share = share // block
    chips = rows_dev // 2
    far = chips // 2
    groups = pairs * seqs
    shard = wq.shape[0]
    weights = w_out.shape[1] + 2 * w_ff1.shape[1]
    n = len(cuts(weights))

    def stream(s):
        g = s // turns
        turn = lax.rem(lax.rem(s, turns) + lax.rem(lax.axis_index("col") + 1, per) * in_share, turns)
        return (lax.rem(g, seqs) * pairs + g // seqs, turn, 0)

    def whole(x):
        n = x.ndim
        return pl.BlockSpec(x.shape, lambda s: (0,) * n, pipeline_mode=pl.Buffered(1))

    blocks = pl.BlockSpec((heads, block, length), stream)
    anywhere = pl.BlockSpec(memory_space=pl.ANY)
    dma = pltpu.SemaphoreType.DMA
    shapes = [
        (cols, total, feat),
        (total, wq.shape[1]),
        (rows_dev, cols, shard, weights),
        (rows_dev,) + wq.shape,
        (cols, 16, feat),
        (cols, share, feat),
        (cols, pairs, share, width),
    ]
    return pl.pallas_call(
        functools.partial(front_kernel, (cols, rows_dev, seqs, heads, pairs, share, block)),
        grid=(groups * turns,),
        in_specs=[whole(x) for x in (tok, wq, w_out, w_ff1, w_ff2, *sides, og, bias)] + [blocks],
        out_specs=[blocks, blocks] + [anywhere] * 7,
        out_shape=[jax.ShapeDtypeStruct(prev.shape, BF16)] * 2 + [jax.ShapeDtypeStruct(s, BF16) for s in shapes],
        scratch_shapes=[
            pltpu.VMEM((cols, total, feat), BF16),
            pltpu.VMEM((rows_dev,) + wq.shape, BF16),
            pltpu.VMEM((total, wq.shape[1]), BF16),
            pltpu.VMEM((length, width), BF16),
            pltpu.VMEM((length, width), BF16),
            pltpu.VMEM((heads, length, width), BF16),
            pltpu.VMEM((groups, length, width), BF16),
            pltpu.VMEM((shard, weights), BF16),
            pltpu.VMEM((16, feat), BF16),
            pltpu.VMEM((rows_dev, cols, shard, weights), BF16),
            dma((5, cols - 1)),
            dma((5, cols - 1)),
            dma((4, far + 1)),
            dma((4, far + 1)),
            dma((2, n, 2, far)),
            dma((2, n, 2, far)),
            dma((2, n, 2, far + 1)),
            dma((2, n, 2, far + 1)),
            dma((groups, per)),
            dma((pairs, cols)),
            dma((5,)),
        ],
        compiler_params=pltpu.CompilerParams(
            collective_id=1, has_side_effects=True, vmem_limit_bytes=60 << 20
        ),
        name="front",
    )(tok, wq, w_out, w_ff1, w_ff2, *sides, og, bias, prev)


def back_kernel(
    dims, proj, wq, tok, datt, outp, dh, gvec, gw, prob, cot,
    pg, out_all, ig, gwo, gqo, gvo,
    datt_s, out_s, dh_s, q_s, k_s, v_s, dq_s, dk_s, dv_s, dp_s,
    own_s, part_s, run_s, run_r, fin_s, fin_r,
    gq_s, gq_p, gq_t, gq_r, ip_s, xi_s, xi_r, vp_s, vs_s, vx_s, vr_s,
    x_send, x_recv, p_send, p_recv, r_send, r_recv, g_send, g_recv, v_send, v_recv, l_sem,
):
    cols, rows_dev, seqs, heads, pairs, share, block = dims
    at = Spot(rows_dev, cols)
    chips, me, core = at.chips, at.me, at.core
    chip = at.row // 2
    half_size = cols // 2
    width = heads * DH
    wide = 3 * width
    length = prob.shape[2]
    per = length // share
    turns = length // block
    in_share = share // block
    shard = gw.shape[3]
    pieces = cuts(gw.shape[4])
    step = pl.program_id(0)
    steps = pairs * seqs * turns
    group = step // turns
    pos = lax.rem(step, turns)
    pair_now = group // seqs
    seq_now = lax.rem(group, seqs)
    turn = lax.rem(pos + lax.rem(me, per) * in_share, turns)
    offs = list(range(1, cols))
    hops = list(range(1, chips))
    far = chips // 2
    total_rows = seqs * length

    def half(k):
        mine = me // half_size
        first = mine if k == 0 else 1 - mine
        return pl.ds(first * half_size, half_size)

    def chip_of(o):
        return chip_at(at.place + o, chips)

    def to_chip(o):
        return (2 * chip_of(o) + core, me)

    def x_copy(kind, j):
        to = at.peer(j)
        src, dst = [
            lambda: (datt.at[to], datt_s.at[me]),
            lambda: (outp.at[to], out_s.at[me]),
            lambda: (dh.at[to], dh_s.at[me]),
            lambda: (fin_s.at[to], fin_r.at[me]),
            lambda: (xi_s.at[j - 1], xi_r.at[j - 1]),
            lambda: (vs_s.at[to], vx_s.at[me]),
        ][kind]()
        return rcopy(src, dst, x_send.at[kind, j - 1], x_recv.at[kind, j - 1], at.col_peer(j))

    def x_got(kind, j):
        came = at.peer(-j)
        src, dst = [
            lambda: (datt.at[came], datt_s.at[came]),
            lambda: (outp.at[came], out_s.at[came]),
            lambda: (dh.at[came], dh_s.at[came]),
            lambda: (fin_s.at[came], fin_r.at[came]),
            lambda: (xi_s.at[j - 1], xi_r.at[j - 1]),
            lambda: (vs_s.at[came], vx_s.at[came]),
        ][kind]()
        return rcopy(src, dst, x_send.at[kind, j - 1], x_recv.at[kind, j - 1], at.col_peer(j))

    def part_copy(o):
        c = chip_of(o)
        return rcopy(gw.at[c, 1 - core], part_s.at[c], p_send.at[o % chips], p_recv.at[o % chips], at.partner)

    def own_load():
        return pltpu.make_async_copy(gw.at[:, core], own_s, l_sem.at[0])

    def locals_():
        return [
            pltpu.make_async_copy(datt.at[me], datt_s.at[me], l_sem.at[1]),
            pltpu.make_async_copy(outp.at[me], out_s.at[me], l_sem.at[2]),
            pltpu.make_async_copy(dh.at[me], dh_s.at[me], l_sem.at[3]),
        ]

    def run_copy(k, p, way, t):
        here = (k, p, way, t - 1)
        return rcopy(run_s.at[here], run_r.at[here], r_send.at[here], r_recv.at[here], at.ring(way))

    waited = set()

    def chip_sum(k, p, o):
        if o % chips not in waited:
            waited.add(o % chips)
            part_copy(o).wait_recv()
        c = chip_of(o)
        return own_s[c, half(k), :, pieces[p]].astype(F32) + part_s[c, half(k), :, pieces[p]].astype(F32)

    def run_step(k, p, t):
        for way in range(2):
            o = depth(chips, k, way) + 1 - t
            if o < 1:
                continue
            value = chip_sum(k, p, o if way == 0 else -o)
            if t > 1:
                run_copy(k, p, way, t - 1).wait_recv()
                value = value + run_r[k, p, way, t - 2].astype(F32)
            run_s[k, p, way, t - 1] = value.astype(BF16)
            run_copy(k, p, way, t).start()

    def run_last(k, p):
        value = chip_sum(k, p, 0)
        for way in range(2):
            d = depth(chips, k, way)
            run_copy(k, p, way, d).wait_recv()
            value = value + run_r[k, p, way, d - 1].astype(F32)
        fin_s[half(k), :, pieces[p]] = value.astype(BF16)

    streams = [(k, p) for p in range(len(pieces)) for k in range(2)]

    def run_round(t, only=None):
        for n, (k, p) in enumerate(streams):
            if only is None or n in only:
                run_step(k, p, t)

    def v_pair():
        return rcopy(gvec, vp_s, v_send.at[0], v_recv.at[0], at.partner)

    def v_chip(o):
        return rcopy(vr_s.at[chip], vr_s.at[chip], v_send.at[o], v_recv.at[o], to_chip(o))

    def v_chip_got(o):
        c = chip_of(-o)
        return rcopy(vr_s.at[c], vr_s.at[c], v_send.at[o], v_recv.at[o], to_chip(o))

    def v_second():
        v_pair().wait_recv()
        vs_s[...] = gvec[...] + vp_s[...]
        for j in offs:
            x_copy(5, j).start()

    def v_third():
        value = vs_s[me]
        for j in offs:
            x_got(5, j).wait_recv()
            value = value + vx_s[at.peer(-j)]
        vr_s[chip] = value
        for o in hops:
            v_chip(o).start()

    def g_pair(j):
        return rcopy(gq_s.at[:, 1 - core], gq_p.at[j], g_send.at[j, 0], g_recv.at[j, 0], at.partner)

    def g_chip(j, o):
        return rcopy(gq_t.at[j, chip_of(o)], gq_r.at[j, chip], g_send.at[j, o], g_recv.at[j, o], to_chip(o))

    def g_chip_got(j, o):
        return rcopy(gq_t.at[j, 0], gq_r.at[j, chip_of(-o)], g_send.at[j, o], g_recv.at[j, o], to_chip(o))

    def g_weight(j):
        slots = chips // cols
        for c in range(cols):
            value = dot_tn(tok[c], dp_s[...]).astype(BF16)
            gq_s[c * slots : (c + 1) * slots, :, :shard, :] = value.reshape(slots, 2, shard, wide)
        sums = col_sum(dp_s[...].astype(F32))
        line = lax.broadcasted_iota(jnp.int32, (16, wide), 0)
        low = jnp.where(line == 0, jnp.broadcast_to(sums, (16, wide)), 0.0).astype(BF16)
        gq_s[:, :, shard:, :] = jnp.broadcast_to(low[None, None], (chips, 2, 16, wide))
        g_pair(j).start()

    def g_pass(j):
        g_pair(j).wait_recv()
        gq_t[j] = (gq_s[:, core].astype(F32) + gq_p[j].astype(F32)).astype(BF16)
        gq_r[j, chip] = gq_t[j, chip]
        for o in hops:
            g_chip(j, o).start()

    def g_last(j):
        for o in hops:
            g_chip_got(j, o).wait_recv()
        value = gq_r[j, 0].astype(F32)
        for c in range(1, chips):
            value = value + gq_r[j, c].astype(F32)
        gqo[:, j * wide : (j + 1) * wide] = value

    chunk = min(512, total_rows)

    def input_part(j, n):
        slots = rows_dev // cols
        w = wq[pl.ds(at.peer(n) * slots, slots), :, j * wide : (j + 1) * wide].reshape(slots * shard, wide)

        def go(i, carry):
            span = pl.ds(pl.multiple_of(i * chunk, chunk), chunk)
            value = dot_nt(dp_s[span, :], w)
            if j > 0:
                value = value + ip_s[n, span, :]
            if j < pairs - 1:
                ip_s[n, span, :] = value
            elif n > 0:
                xi_s[n - 1, span, :] = value.astype(BF16)
            else:
                ip_s[0, span, :] = value
            return carry

        lax.fori_loop(0, total_rows // chunk, go, 0)

    @pl.when(step == 0)
    def _():
        greet(
            [at.ring(0), at.ring(1), at.partner]
            + [at.col_peer(j) for j in offs]
            + [to_chip(o) for o in hops if o not in (1, chips - 1)]
        )
        for j in offs:
            x_copy(0, j).start()
        own_load().start()
        v_pair().start()
        order = [far] + [s * o for o in range(far - 1, 0, -1) for s in (1, -1)] + [0]
        for o in order:
            part_copy(o).start()
        for c in locals_():
            c.start()
        for c in locals_():
            c.wait()
        if seqs > 1:
            for j in offs:
                x_got(0, j).wait_recv()

    if seqs == 1:

        @pl.when(step == in_share)
        def _():
            for j in offs:
                x_got(0, j).wait_recv()

    @pl.when(pos == 0)
    def _():
        for pair in range(pairs):

            @pl.when(pair_now == pair)
            def _():
                here = proj[pl.ds(pl.multiple_of(seq_now * length, length), length), :]
                q_s[...] = part_of(here, pair, heads, 0) * jnp.asarray(0.125, BF16)
                k = part_of(here, pair, heads, 1)
                for i in range(heads):
                    k_s[i] = pick(k, i, width)
                v_s[...] = part_of(here, pair, heads, 2)

        dk_s[...] = jnp.zeros_like(dk_s)
        dv_s[...] = jnp.zeros_like(dv_s)

    jobs = {
        0: [lambda: own_load().wait(), lambda: run_round(1)],
        1: [v_second] + [lambda kind=kind, j=j: x_copy(kind, j).start() for kind in (1, 2) for j in offs],
        2: [lambda: run_round(2, (0, 1))],
        3: [lambda: run_round(2, (2,)), v_third],
        4: [lambda: run_round(2, (3,)), lambda: run_round(3, (0,))],
        5: [lambda: run_round(3, (1,))],
        6: [lambda: run_round(3, (2, 3))],
        7: [lambda: run_round(4, (0,))],
    }

    def spot(n):
        return (n * steps) // 8

    for n, todo in jobs.items():

        @pl.when(step == spot(n))
        def _(todo=todo):
            for job in todo:
                job()

    @pl.when((step == steps // pairs) & (pairs > 1))
    def _():
        if pairs > 1:
            g_pass(0)

    rows_now = pl.ds(pl.multiple_of(turn * block, block), block)
    q_rows = q_s[rows_now, :]
    source = seq_now * per + turn // in_share
    inside = pl.ds(pl.multiple_of(lax.rem(turn, in_share) * block, block), block)
    dq = dk = dv = None
    for pair in range(pairs):

        @pl.when(pair_now == pair)
        def _():
            dq = dk = dv = None
            d_rows = datt_s[source, inside, pair * width : (pair + 1) * width]
            for i in range(heads):
                d_one = pick(d_rows, i, width)
                d_probs = dot_nt(d_one, v_s[...])
                p = prob[i]
                p_wide = p.astype(F32)
                delta = jnp.sum(d_probs * p_wide, axis=1, keepdims=True)
                low = (p_wide * (d_probs - delta) + cot[i].astype(F32)).astype(BF16)
                pg[i] = low
                a = dot_nn(low, k_s[i])
                b = dot_tn(pick(q_rows, i, width), low)
                c = dot_tn(d_one, p)
                dq = a if dq is None else dq + a
                dk = b if dk is None else dk + b
                dv = c if dv is None else dv + c
            dq_s[rows_now, :] = (dq * 0.125).astype(BF16)
            dk_s[...] += dk
            dv_s[...] += dv

    @pl.when(pos == turns - 1)
    def _():
        parts = [dq_s[...], dk_s[...].T.astype(BF16), dv_s[...].T.astype(BF16)]
        here = pl.ds(pl.multiple_of(seq_now * length, length), length)
        for i in range(heads):
            dp_s[here, i * 3 * DH : (i + 1) * 3 * DH] = jnp.concatenate([p[:, i * DH : (i + 1) * DH] for p in parts], axis=1)

    for j in range(pairs - 1):

        @pl.when(step == (j + 1) * (steps // pairs) - 1)
        def _():
            g_weight(j)
            for n in range(cols):
                input_part(j, n)

    @pl.when(step == steps - 1)
    def _():
        last = pairs - 1
        for j in offs:
            input_part(last, j)
            x_copy(4, j).start()
        if pairs > 1:
            g_pair(last - 1).wait_send()
        run_round(4, (1, 2, 3))
        g_weight(last)
        for t in range(5, far + 1):
            run_round(t)
        input_part(last, 0)
        g_pass(last)
        for j in offs:
            x_got(1, j).wait_recv()
            x_got(2, j).wait_recv()
        keep = pltpu.make_async_copy(out_s, out_all, l_sem.at[1])
        keep.start()
        for k, p in streams:
            run_last(k, p)
        for j in offs:
            x_copy(3, j).start()
        for o in hops:
            v_chip_got(o).wait_recv()
        value = vr_s[0]
        for c in range(1, chips):
            value = value + vr_s[c]
        gvo[...] = value
        for j in range(pairs):
            g_last(j)
        for j in offs:
            x_got(4, j).wait_recv()

        def finish(i, carry):
            c = i // (share // min(share, chunk))
            rows = min(share, chunk)
            inner = pl.ds(pl.multiple_of(lax.rem(i, share // rows) * rows, rows), rows)
            span = pl.ds(pl.multiple_of(i * rows, rows), rows)
            value = ip_s[0, span, :] + dh_s[c, inner, :].astype(F32)
            for j in offs:
                value = value + xi_r[j - 1, span, :].astype(F32)
            ig[span, :] = value.astype(BF16)
            return carry

        lax.fori_loop(0, total_rows // min(share, chunk), finish, 0)
        value = fin_s[me].astype(F32)
        for j in offs:
            x_got(3, j).wait_recv()
            value = value + fin_r[at.peer(-j)].astype(F32)
        gwo[...] = value
        keep.wait()
        for kind in range(6):
            for j in offs:
                x_copy(kind, j).wait_send()
        for o in range(chips):
            part_copy(o).wait_send()
        for k in range(2):
            for way in range(2):
                for t in range(1, depth(chips, k, way) + 1):
                    for p in range(len(pieces)):
                        run_copy(k, p, way, t).wait_send()
        v_pair().wait_send()
        for o in hops:
            v_chip(o).wait_send()
        g_pair(last).wait_send()
        for j in range(pairs):
            for o in hops:
                g_chip(j, o).wait_send()


def back(cols, rows_dev, seqs, head_count, proj, wq, tok, datt, outp, dh, gvec, gw, prob, cot):
    heads = min(2, head_count)
    pairs = head_count // heads
    _, total, feat = tok.shape
    share = total // cols
    length = prob.shape[-1]
    width = heads * DH
    wide = 3 * width
    block = min(256, share)
    turns = length // block
    per = length // share
    in_share = share // block
    chips = rows_dev // 2
    far = chips // 2
    shard, weights = gw.shape[2:]
    half_size = cols // 2
    n = len(cuts(weights))
    gw = gw.reshape(chips, 2, cols, shard, weights)

    def stream(s):
        g = s // turns
        turn = lax.rem(lax.rem(s, turns) + lax.rem(lax.axis_index("col"), per) * in_share, turns)
        return (lax.rem(g, seqs) * pairs + g // seqs, turn, 0)

    def whole(shape):
        n = len(shape)
        return pl.BlockSpec(shape, lambda s: (0,) * n, pipeline_mode=pl.Buffered(1))

    blocks = pl.BlockSpec((heads, block, length), stream)
    anywhere = pl.BlockSpec(memory_space=pl.ANY)
    dma = pltpu.SemaphoreType.DMA
    outs = [
        jax.ShapeDtypeStruct(prob.shape, BF16),
        jax.ShapeDtypeStruct((cols, share, feat), BF16),
        jax.ShapeDtypeStruct((total, feat), BF16),
        jax.ShapeDtypeStruct((shard, weights), F32),
        jax.ShapeDtypeStruct((shard + 16, wq.shape[2]), F32),
        jax.ShapeDtypeStruct(gvec.shape[1:], F32),
    ]
    return pl.pallas_call(
        functools.partial(back_kernel, (cols, rows_dev, seqs, heads, pairs, share, block)),
        grid=(pairs * seqs * turns,),
        in_specs=[whole(x.shape) for x in (proj, wq, tok, datt, outp, dh, gvec)] + [anywhere, blocks, blocks],
        out_specs=[blocks, anywhere] + [whole(o.shape) for o in outs[2:]],
        out_shape=outs,
        scratch_shapes=[
            pltpu.VMEM(datt.shape, BF16),
            pltpu.VMEM(outp.shape, BF16),
            pltpu.VMEM(dh.shape, BF16),
            pltpu.VMEM((length, width), BF16),
            pltpu.VMEM((heads, length, width), BF16),
            pltpu.VMEM((length, width), BF16),
            pltpu.VMEM((length, width), BF16),
            pltpu.VMEM((width, length), F32),
            pltpu.VMEM((width, length), F32),
            pltpu.VMEM((total, wide), BF16),
            pltpu.VMEM((chips, cols, shard, weights), BF16),
            pltpu.VMEM((chips, cols, shard, weights), BF16),
            pltpu.VMEM((2, n, 2, far, half_size, shard, weights // n), BF16),
            pltpu.VMEM((2, n, 2, far, half_size, shard, weights // n), BF16),
            pltpu.VMEM((cols, shard, weights), BF16),
            pltpu.VMEM((cols, shard, weights), BF16),
            pltpu.VMEM((chips, 2, shard + 16, wide), BF16),
            pltpu.VMEM((pairs, chips, shard + 16, wide), BF16),
            pltpu.VMEM((pairs, chips, shard + 16, wide), BF16),
            pltpu.VMEM((pairs, chips, shard + 16, wide), BF16),
            pltpu.VMEM((cols if pairs > 1 else 1, total, feat), F32),
            pltpu.VMEM((cols - 1, total, feat), BF16),
            pltpu.VMEM((cols - 1, total, feat), BF16),
            pltpu.VMEM(gvec.shape, F32),
            pltpu.VMEM(gvec.shape, F32),
            pltpu.VMEM(gvec.shape, F32),
            pltpu.VMEM((chips,) + gvec.shape[1:], F32),
            dma((6, cols - 1)),
            dma((6, cols - 1)),
            dma((chips,)),
            dma((chips,)),
            dma((2, n, 2, far)),
            dma((2, n, 2, far)),
            dma((pairs, chips)),
            dma((pairs, chips)),
            dma((chips,)),
            dma((chips,)),
            dma((4,)),
        ],
        compiler_params=pltpu.CompilerParams(
            collective_id=2, has_side_effects=True, vmem_limit_bytes=62 << 20
        ),
        name="back",
    )(proj, wq, tok, datt, outp, dh, gvec, gw, prob, cot)


def finish_kernel(cols, pg_in, out_in, ig_in, gw, gq, gv, pg, out, ig, wq, bq, wo, bo, n1g, n1s, w1, b1, w2, b2, n2g, n2s, bounce, in_sem, out_sem):
    slots = bounce.shape[0]
    takes = [pltpu.make_async_copy(pg_in.at[n], bounce.at[n], in_sem.at[n]) for n in range(slots)]
    puts = [pltpu.make_async_copy(bounce.at[n], pg.at[n], out_sem.at[n]) for n in range(slots)]
    for c in takes:
        c.start()
    shard = wq.shape[0]
    hw, fw = wo.shape[1], w1.shape[1]
    feat = out.shape[1]
    for c in range(cols):
        out[c * out_in.shape[1] : (c + 1) * out_in.shape[1], :] = out_in[c]
    ig[...] = ig_in[...]
    for n in range(slots // 2):
        takes[n].wait()
        puts[n].start()
    wq[...] = gq[:shard]
    bq[...] = gq[shard : shard + 1].reshape(-1)
    wo[...] = gw[:, :hw]
    w1[...] = gw[:, hw : hw + fw]
    w2[...] = gw[:, hw + fw :]
    for i, ref in enumerate((bo, n1g, n1s, b2, n2g, n2s)):
        ref[...] = gv[i : i + 1].reshape(-1)
    b1[...] = jnp.concatenate([gv[6 + i : 7 + i] for i in range(fw // feat)], axis=1).reshape(-1)
    for n in range(slots // 2, slots):
        takes[n].wait()
        puts[n].start()
    for c in puts:
        c.wait()


def finish(cols, pg, out, ig, gw, gq, gv, hw, fw):
    slots = 8
    pieces = (slots, pg.shape[0] * pg.shape[1] // slots, pg.shape[2])
    total, feat = ig.shape
    shard = gw.shape[0]
    vmem = pl.BlockSpec(memory_space=pltpu.VMEM)
    anywhere = pl.BlockSpec(memory_space=pl.ANY)

    def f32(*shape):
        return jax.ShapeDtypeStruct(shape, F32)

    outs = [
        jax.ShapeDtypeStruct(pieces, BF16),
        jax.ShapeDtypeStruct(ig.shape, BF16),
        jax.ShapeDtypeStruct(ig.shape, BF16),
        f32(shard, gq.shape[1]),
        f32(gq.shape[1]),
        f32(shard, hw),
        f32(feat),
        f32(feat),
        f32(feat),
        f32(shard, fw),
        f32(fw),
        f32(shard, fw),
        f32(feat),
        f32(feat),
        f32(feat),
    ]
    return pl.pallas_call(
        functools.partial(finish_kernel, cols),
        out_shape=outs,
        in_specs=[anywhere] + [vmem] * 5,
        out_specs=[anywhere] + [vmem] * 14,
        scratch_shapes=[
            pltpu.VMEM(pieces, BF16),
            pltpu.SemaphoreType.DMA((slots,)),
            pltpu.SemaphoreType.DMA((slots,)),
        ],
        compiler_params=pltpu.CompilerParams(vmem_limit_bytes=60 << 20),
        name="finish",
    )(pg.reshape(pieces), out, ig, gw, gq, gv)


def per_device(
    cols,
    row_count,
    tokens,
    prev_logits,
    qkv_weight,
    qkv_bias,
    out_weight,
    out_bias,
    norm1_gain,
    norm1_shift,
    ff1_weight,
    ff1_bias,
    ff2_weight,
    ff2_bias,
    norm2_gain,
    norm2_shift,
    out_grad,
    logit_grad,
):
    seqs, head_count, length, _ = prev_logits.shape
    total, feat = tokens.shape
    share = total // cols
    rows = min(256, length)
    rows_dev = row_count
    hidden = ff1_weight.shape[1]
    sides = (out_bias, norm1_gain, norm1_shift, ff2_bias, norm2_gain, norm2_shift, ff1_bias)
    prev = prev_logits.reshape(seqs * head_count, length, length)
    cot = logit_grad.reshape(seqs * head_count, length, length)
    raw, prob, tok_all, proj, wf_all, wq_all, vec_all, og_all, att_all = front(
        cols, rows_dev, seqs, head_count, tokens, qkv_weight, out_weight.T, ff1_weight, ff2_weight.T, sides, out_grad, qkv_bias, prev
    )
    out, dh, datt, gw, gvec, raw = middle(tok_all, att_all, og_all, wf_all, vec_all, raw)

    prev_grad, output, input_grad, gw, gq, gv = back(
        cols, rows_dev, seqs, head_count, proj, wq_all, tok_all, datt, out, dh, gvec, gw, prob, cot
    )
    prev_grad, output, input_grad, *rest = finish(
        cols, prev_grad, output, input_grad, gw, gq, gv, out_weight.shape[0], hidden
    )
    rest[2] = rest[2].T
    rest[8] = rest[8].T
    return output, raw.reshape(prev_logits.shape), input_grad, prev_grad.reshape(prev_logits.shape), *rest


def solution(mesh):
    in_specs = (
        P("row", "col"),
        P("row", "col", None, None),
        P("row", "col"),
        P("col"),
        P("col", "row"),
        P("col"),
        P("col"),
        P("col"),
        P("row", "col"),
        P("col"),
        P("col", "row"),
        P("col"),
        P("col"),
        P("col"),
        P("row", "col"),
        P("row", "col", None, None),
    )
    out_specs = (
        P("row", "col"),
        P("row", "col", None, None),
        P("row", "col"),
        P("row", "col", None, None),
        P("row", "col"),
        P("col"),
        P("col", "row"),
        P("col"),
        P("col"),
        P("col"),
        P("row", "col"),
        P("col"),
        P("col", "row"),
        P("col"),
        P("col"),
        P("col"),
    )
    return jax.shard_map(
        functools.partial(per_device, mesh.shape["col"], mesh.shape["row"]),
        mesh=mesh,
        in_specs=in_specs,
        out_specs=out_specs,
        check_vma=False,
    )
```

```python
import functools
import math

import jax
import jax.numpy as jnp
from jax import lax
from jax.experimental import pallas as pl
from jax.experimental.pallas import tpu as pltpu
from jax.sharding import PartitionSpec as P

DH = 64
F32 = jnp.float32
BF16 = jnp.bfloat16
norm_eps = 1e-06
root_half = 0.7071067811865476
inv_root_two_pi = 0.3989422804014327
NT = (((1,), (1,)), ((), ()))
TN = (((0,), (0,)), ((), ()))


def dot_nn(a, b):
    return jnp.dot(a, b, preferred_element_type=F32)


def dot_nt(a, b):
    return lax.dot_general(a, b, NT, preferred_element_type=F32)


def dot_tn(a, b):
    return lax.dot_general(a, b, TN, preferred_element_type=F32)


def pick(value, index, width):
    if width == DH:
        return value
    lane = lax.broadcasted_iota(jnp.int32, value.shape, 1)
    keep = (lane >= index * DH) & (lane < (index + 1) * DH)
    return jnp.where(keep, value, jnp.zeros_like(value))


def part_of(proj, pair, heads, part):
    pieces = [
        proj[:, (pair * heads + i) * 3 * DH + part * DH :][:, :DH] for i in range(heads)
    ]
    return pieces[0] if heads == 1 else jnp.concatenate(pieces, axis=1)


def forward_block(q_rows, k_all, v_masked, prev, width):
    raws, probs, total = [], [], None
    for i in range(width // DH):
        scores = dot_nt(pick(q_rows, i, width), k_all) + prev[i].astype(F32)
        raws.append(scores.astype(BF16))
        exponent = jnp.exp(scores - jnp.max(scores, axis=1, keepdims=True))
        scale = 1.0 / jnp.sum(exponent, axis=1, keepdims=True)
        prob = (exponent * scale).astype(BF16)
        probs.append(prob)
        out = dot_nn(prob, v_masked[i])
        total = out if total is None else total + out
    return raws, probs, total


def normalize(hidden):
    width = hidden.shape[1]
    center = hidden - jnp.sum(hidden, axis=1, keepdims=True) * (1.0 / width)
    inv_std = lax.rsqrt(jnp.sum(center * center, axis=1, keepdims=True) * (1.0 / width) + norm_eps)
    return center * inv_std, inv_std


def norm_back(scaled, xhat, inv_std):
    width = scaled.shape[1]
    mean_grad = jnp.sum(scaled, axis=1, keepdims=True) * (1.0 / width)
    mean_cross = jnp.sum(scaled * xhat, axis=1, keepdims=True) * (1.0 / width)
    return inv_std * (scaled - mean_grad - xhat * mean_cross)


def col_sum(value):
    return jnp.sum(value, axis=0, keepdims=True)


def middle_kernel(
    dims, tok_ref, att_ref, og_ref, vec_ref, w_in, raw_in,
    out_ref, dh_ref, datt_ref, gvec_ref, gw_out, raw_out,
    act_s, slope_s, w_ref, gw_ref, bounce, w_sem, g_sem, in_sem, out_sem,
):
    cols, share, hw, fw = dims
    feat = vec_ref.shape[2]
    pairs, width = att_ref.shape[1], att_ref.shape[3]
    slots, rows_dev = bounce.shape[0], w_ref.shape[0]
    shard = w_ref.shape[2]
    cut = min(512, fw)
    me = lax.axis_index("col")

    total = w_ref.shape[3]
    ranges = [(0, hw), (hw, fw), (hw + fw, fw)] if hw % 128 == 0 and fw % 128 == 0 else [(0, total)]

    def columns(ref, n):
        return ref.at[:, :, :, pl.ds(*ranges[n])]

    loads = [pltpu.make_async_copy(columns(w_in, n), columns(w_ref, n), w_sem.at[n]) for n in range(len(ranges))]
    stores = [pltpu.make_async_copy(columns(gw_ref, n), columns(gw_out, n), g_sem.at[n]) for n in range(len(ranges))]
    split = len(ranges) == 3
    for c in loads:
        c.start()
    loads[0].wait()
    takes = [pltpu.make_async_copy(raw_in.at[n], bounce.at[n], in_sem.at[n]) for n in range(slots)]
    puts = [pltpu.make_async_copy(bounce.at[n], raw_out.at[n], out_sem.at[n]) for n in range(slots)]
    for c in takes:
        c.start()

    def side(ref, i):
        return jnp.concatenate([ref[c, i : i + 1] for c in range(cols)], axis=1).astype(F32)

    def weight(c, a, b):
        return w_ref[:, c, :, a:b].reshape(rows_dev * shard, b - a)

    def put_weight(c, a, b, value):
        gw_ref[:, c, :, a:b] = value.astype(BF16).reshape(rows_dev, shard, b - a)

    own = pl.ds(pl.multiple_of(me * share, share), share)
    out_bias, gain1, shift1, ff2_bias, gain2, shift2 = (side(vec_ref, i) for i in range(6))
    tok = jnp.concatenate([tok_ref[c, own, :] for c in range(cols)], axis=1)

    hidden1 = tok.astype(F32) + out_bias
    for c in range(cols):
        for j in range(pairs):
            hidden1 = hidden1 + dot_nt(att_ref[c, j], weight(c, j * width, (j + 1) * width))
    xhat1, inv1 = normalize(hidden1)
    normed1 = xhat1 * gain1 + shift1
    low1 = normed1.astype(BF16)

    chunks = [(c, o) for c in range(cols) for o in range(0, fw, cut)]
    hidden2 = normed1 + ff2_bias
    if split:
        loads[1].wait()
        loads[2].wait()
    for c, o in chunks:
        at = c * fw + o
        bias = jnp.concatenate([vec_ref[c, 6 + (o + i) // feat : 7 + (o + i) // feat] for i in range(0, cut, feat)], axis=1)
        inner = dot_nn(low1, weight(c, hw + o, hw + o + cut)) + bias.astype(F32)
        half = 0.5 + 0.5 * lax.erf(inner * root_half)
        act = (inner * half).astype(BF16)
        act_s[:, at : at + cut] = act
        slope_s[:, at : at + cut] = half + inner * inv_root_two_pi * jnp.exp(-0.5 * inner * inner)
        hidden2 = hidden2 + dot_nt(act, weight(c, hw + fw + o, hw + fw + o + cut))
    for n in range(slots):
        takes[n].wait()
        puts[n].start()
    xhat2, inv2 = normalize(hidden2)
    output = (xhat2 * gain2 + shift2).astype(BF16)

    og = jnp.concatenate([og_ref[c] for c in range(cols)], axis=1).astype(F32)
    d_hidden2 = norm_back(og * gain2, xhat2, inv2)
    low2 = d_hidden2.astype(BF16)
    rows = [None] * 6
    rows[4] = col_sum(og * xhat2)
    rows[5] = col_sum(og)
    rows[3] = col_sum(low2.astype(F32))
    low1_t = low1.T
    low2_t = low2.T
    d_normed1 = d_hidden2
    for c, o in chunks:
        at = c * fw + o
        d_act = dot_nn(low2, weight(c, hw + fw + o, hw + fw + o + cut))
        d_inner = (d_act * slope_s[:, at : at + cut]).astype(BF16)
        d_normed1 = d_normed1 + dot_nt(d_inner, weight(c, hw + o, hw + o + cut))
        put_weight(c, hw + o, hw + o + cut, dot_nn(low1_t, d_inner))
        put_weight(c, hw + fw + o, hw + fw + o + cut, dot_nn(low2_t, act_s[:, at : at + cut]))
        sums = col_sum(d_inner.astype(F32))
        for i in range(0, cut, feat):
            gvec_ref[c, 6 + (o + i) // feat : 7 + (o + i) // feat] = sums[:, i : i + feat]

    if split:
        stores[1].start()
        stores[2].start()
    rows[1] = col_sum(d_normed1 * xhat1)
    rows[2] = col_sum(d_normed1)
    d_hidden1 = norm_back(d_normed1 * gain1, xhat1, inv1)
    low = d_hidden1.astype(BF16)
    rows[0] = col_sum(low.astype(F32))
    low_t = low.T
    spare = gvec_ref.shape[1] - 6 - fw // feat
    for c in range(cols):
        for j in range(pairs):
            put_weight(c, j * width, (j + 1) * width, dot_nn(low_t, att_ref[c, j]))
        datt_ref[c] = dot_nn(low, weight(c, 0, hw)).astype(BF16)
        span = slice(c * feat, (c + 1) * feat)
        out_ref[c] = output[:, span]
        dh_ref[c] = low[:, span]
        for i in range(6):
            gvec_ref[c, i : i + 1] = rows[i][:, span]
        if spare:
            gvec_ref[c, 6 + fw // feat :] = jnp.zeros((spare, feat), F32)
    stores[0].start()
    for c in puts:
        c.wait()
    for c in stores:
        c.wait()


def middle(tok, att, og, w, vec, raw):
    rows_dev, cols, shard, _ = w.shape
    feat = tok.shape[2]
    share = og.shape[1]
    hw = att.shape[1] * att.shape[3]
    fw = (w.shape[3] - hw) // 2
    slots = 4
    pieces = (slots, raw.shape[0] * raw.shape[1] // slots, raw.shape[2])
    vmem = pl.BlockSpec(memory_space=pltpu.VMEM)
    anywhere = pl.BlockSpec(memory_space=pl.ANY)
    results = pl.pallas_call(
        functools.partial(middle_kernel, (cols, share, hw, fw)),
        out_shape=[
            jax.ShapeDtypeStruct((cols, share, feat), BF16),
            jax.ShapeDtypeStruct((cols, share, feat), BF16),
            jax.ShapeDtypeStruct((cols, share, hw), BF16),
            jax.ShapeDtypeStruct(vec.shape, F32),
            jax.ShapeDtypeStruct(w.shape, BF16),
            jax.ShapeDtypeStruct(pieces, BF16),
        ],
        in_specs=[vmem] * 4 + [anywhere] * 2,
        out_specs=[vmem] * 4 + [anywhere] * 2,
        scratch_shapes=[
            pltpu.VMEM((share, cols * fw), BF16),
            pltpu.VMEM((share, cols * fw), F32),
            pltpu.VMEM(w.shape, BF16),
            pltpu.VMEM(w.shape, BF16),
            pltpu.VMEM(pieces, BF16),
            pltpu.SemaphoreType.DMA((3,)),
            pltpu.SemaphoreType.DMA((3,)),
            pltpu.SemaphoreType.DMA((slots,)),
            pltpu.SemaphoreType.DMA((slots,)),
        ],
        compiler_params=pltpu.CompilerParams(vmem_limit_bytes=60 << 20),
        name="middle",
    )(tok, att, og, vec, w, raw.reshape(pieces))
    return *results[:-1], results[-1].reshape(raw.shape)


MESH = pl.DeviceIdType.MESH


def chip_at(place, chips):
    place = lax.rem(place + 2 * chips, chips)
    return jnp.where(place < chips // 2, 2 * place, 2 * (chips - 1 - place) + 1)


def place_of(chip, chips):
    return jnp.where(lax.rem(chip, 2) == 0, chip // 2, chips - 1 - chip // 2)


class Spot:
    def __init__(self, devices_row, cols):
        self.cols = cols
        self.chips = devices_row // 2
        self.row = lax.axis_index("row")
        self.me = lax.axis_index("col")
        self.core = lax.rem(self.row, 2)
        self.place = place_of(self.row // 2, self.chips)
        self.partner = (self.row + 1 - 2 * self.core, self.me)

    def row_at(self, offset):
        return 2 * chip_at(self.place + offset, self.chips) + self.core

    def ring(self, way):
        return (self.row_at(1 if way == 0 else -1), self.me)

    def peer(self, j):
        return lax.rem(self.me + j + self.cols, self.cols)

    def col_peer(self, j):
        return (self.row, self.peer(j))


def greet(others):
    barrier = pltpu.get_barrier_semaphore()
    for other in others:
        pl.semaphore_signal(barrier, inc=1, device_id=other, device_id_type=MESH)
    pl.semaphore_wait(barrier, len(others))


def rcopy(src, dst, send, recv, to):
    return pltpu.make_async_remote_copy(
        src_ref=src, dst_ref=dst, send_sem=send, recv_sem=recv, device_id=to, device_id_type=MESH
    )


def cuts(weights):
    n = 2 if weights % 256 == 0 else 1
    return [pl.ds(i * (weights // n), weights // n) for i in range(n)]


def depth(chips, k, way):
    return chips // 2 if k == way else chips // 2 - 1


def front_kernel(
    dims, tok, wq, w_out, w_ff1, w_ff2, side0, side1, side2, side3, side4, side5, side6, og, bias, prev, raw, prob, tok_all, proj_all, wf_all, wq_all, vec_all, og_all, att_all,
    tok_s, wq_s, proj_s, q_s, k_s, v_s, att_s, wf, vec, wf_v,
    x_send, x_recv, q_send, q_recv, f_send, f_recv, p_send, p_recv, a_send, a_recv, l_sem,
):
    cols, rows_dev, seqs, heads, pairs, share, block = dims
    at = Spot(rows_dev, cols)
    chips, me, row = at.chips, at.me, at.row
    half_size = cols // 2
    width = heads * DH
    length = prev.shape[2]
    per = length // share
    turns = length // block
    in_share = share // block
    step = pl.program_id(0)
    steps = pairs * seqs * turns
    group = step // turns
    pos = lax.rem(step, turns)
    pair_now = group // seqs
    seq_now = lax.rem(group, seqs)
    turn = lax.rem(pos + lax.rem(me + 1, per) * in_share, turns)
    offs = [j for j in range(1, cols)]
    far = chips // 2
    pieces = cuts(wf.shape[1])
    kinds = ("tok", "tok2", "wf", "vec", "og")
    first = pl.ds(0, tok.shape[0] // 2)
    second = pl.ds(tok.shape[0] // 2, tok.shape[0] // 2)

    def half(k):
        mine = me // half_size
        first = mine if k == 0 else 1 - mine
        return pl.ds(first * half_size, half_size)

    def off(way, h):
        return -h if way == 0 else h

    def q_hop(way, h):
        r = at.row_at(off(way, h - 1))
        src = wq if h == 1 else wq_s.at[r]
        return rcopy(src, wq_s.at[r], q_send.at[way, h - 1], q_recv.at[way, h - 1], at.ring(way))

    def q_got(way, h):
        r = at.row_at(off(way, h))
        return rcopy(wq, wq_s.at[r], q_send.at[way, h - 1], q_recv.at[way, h - 1], at.ring(way))

    def q_pair(way, h, mine=True):
        r = at.row_at(off(way, h))
        src = wq if h == 0 else wq_s.at[r]
        if not mine:
            r = r + 1 - 2 * at.core
        return rcopy(src, wq_s.at[r], q_send.at[2 + way, h], q_recv.at[2 + way, h], at.partner)

    def f_hop(k, p, way, h):
        part = wf_v.at[at.row_at(off(way, h - 1)), half(k), :, pieces[p]]
        return rcopy(part, part, f_send.at[k, p, way, h - 1], f_recv.at[k, p, way, h - 1], at.ring(way))

    def f_got(k, p, way, h):
        part = wf_v.at[at.row_at(off(way, h)), half(k), :, pieces[p]]
        return rcopy(part, part, f_send.at[k, p, way, h - 1], f_recv.at[k, p, way, h - 1], at.ring(way))

    def f_pair(k, p, way, h, mine=True):
        r = at.row_at(off(way, h))
        if not mine:
            r = r + 1 - 2 * at.core
        part = wf_v.at[r, half(k), :, pieces[p]]
        return rcopy(part, part, p_send.at[k, p, way, h], p_recv.at[k, p, way, h], at.partner)

    def f_own(k, p):
        f_hop(k, p, 0, 1).start()
        f_hop(k, p, 1, 1).start()
        f_pair(k, p, 0, 0).start()

    def x_copy(kind, j):
        to = at.peer(j)
        src, dst = {
            "tok": (tok.at[first], tok_s.at[me, first]),
            "tok2": (tok.at[second], tok_s.at[me, second]),
            "wf": (wf, wf_v.at[row, me]),
            "vec": (vec, vec_all.at[me]),
            "og": (og.at[pl.ds(pl.multiple_of(to * share, share), share)], og_all.at[me]),
        }[kind]
        n = kinds.index(kind)
        return rcopy(src, dst, x_send.at[n, j - 1], x_recv.at[n, j - 1], at.col_peer(j))

    def x_got(kind, j):
        came = at.peer(-j)
        src, dst = {
            "tok": (tok.at[first], tok_s.at[came, first]),
            "tok2": (tok.at[second], tok_s.at[came, second]),
            "wf": (wf, wf_v.at[row, came]),
            "vec": (vec, vec_all.at[came]),
            "og": (og.at[pl.ds(0, share)], og_all.at[came]),
        }[kind]
        n = kinds.index(kind)
        return rcopy(src, dst, x_send.at[n, j - 1], x_recv.at[n, j - 1], at.col_peer(j))

    def locals_():
        own = pl.ds(pl.multiple_of(me * share, share), share)
        return [
            pltpu.make_async_copy(wf, wf_v.at[row, me], l_sem.at[0]),
            pltpu.make_async_copy(wq, wq_s.at[row], l_sem.at[1]),
            pltpu.make_async_copy(tok, tok_s.at[me], l_sem.at[2]),
            pltpu.make_async_copy(vec, vec_all.at[me], l_sem.at[3]),
            pltpu.make_async_copy(og.at[own], og_all.at[me], l_sem.at[4]),
        ]

    def saves():
        return [
            pltpu.make_async_copy(tok_s, tok_all, l_sem.at[0]),
            pltpu.make_async_copy(wq_s, wq_all, l_sem.at[1]),
            pltpu.make_async_copy(proj_s, proj_all, l_sem.at[2]),
        ]

    def handle(k, h, only=None):
        for p in range(len(pieces)) if only is None else only:
            for way in range(2):
                if h <= depth(chips, k, way):
                    f_got(k, p, way, h).wait_recv()
                    if h < depth(chips, k, way):
                        f_hop(k, p, way, h + 1).start()
                    f_pair(k, p, way, h).start()

    @pl.when(step == 0)
    def _():
        hw, fw = w_out.shape[1], w_ff1.shape[1]
        wf[:, :hw] = w_out[...]
        wf[:, hw : hw + fw] = w_ff1[...]
        wf[:, hw + fw :] = w_ff2[...]
        feat = vec.shape[1]
        vec[...] = jnp.zeros_like(vec)
        for i, ref in enumerate((side0, side1, side2, side3, side4, side5)):
            vec[i : i + 1, :] = ref[...].reshape(1, feat)
        long = side6[...].reshape(1, fw)
        for i in range(fw // feat):
            vec[6 + i : 7 + i, :] = long[:, i * feat : (i + 1) * feat]
        greet([at.ring(0), at.ring(1), at.partner] + [at.col_peer(j) for j in offs])
        q_hop(0, 1).start()
        q_hop(1, 1).start()
        for kind in ("wf", "tok", "tok2", "vec"):
            for j in offs:
                x_copy(kind, j).start()
        q_pair(0, 0).start()
        for c in locals_():
            c.start()
        for c in locals_():
            c.wait()
        if cols > 2:
            for j in offs:
                x_got("wf", j).wait_recv()
        for h in range(1, far + 1):
            for way in range(2):
                if h <= depth(chips, 0, way):
                    q_got(way, h).wait_recv()
                    if h < depth(chips, 0, way):
                        q_hop(way, h + 1).start()
                    q_pair(way, h).start()
            if h == 1:
                for p in range(len(pieces)):
                    f_own(0, p)
            if h == 3:
                if cols == 2:
                    for j in offs:
                        x_got("wf", j).wait_recv()
                for p in range(len(pieces)):
                    f_own(1, p)
            if h == 3:
                handle(0, 1)
        for j in offs:
            x_copy("og", j).start()
        handle(1, 1)
        for way in range(2):
            for h in range(0 if way == 0 else 1, depth(chips, 0, way) + 1):
                q_pair(way, h, mine=False).wait_recv()
        for j in offs:
            x_got("tok", j).wait_recv()
        rows = wq_s.shape[0] // cols
        chunk = min(512, tok.shape[0])

        def project(i, carry):
            span = pl.ds(pl.multiple_of(i * chunk, chunk), chunk)

            @pl.when(i == tok.shape[0] // chunk // 2)
            def _():
                for j in offs:
                    x_got("tok2", j).wait_recv()

            total = bias[...].reshape(1, -1).astype(F32)
            for c in range(cols):
                w = wq_s[c * rows : (c + 1) * rows].reshape(-1, wq_s.shape[2])
                total = total + dot_nn(tok_s[c, span, :], w)
            proj_s[span, :] = total.astype(BF16)
            return carry

        lax.fori_loop(0, tok.shape[0] // chunk, project, 0)

    @pl.when(pos == 0)
    def _():
        for pair in range(pairs):

            @pl.when(pair_now == pair)
            def _():
                proj = proj_s[pl.ds(pl.multiple_of(seq_now * length, length), length), :]
                q_s[...] = part_of(proj, pair, heads, 0) * jnp.asarray(0.125, BF16)
                k_s[...] = part_of(proj, pair, heads, 1)
                v = part_of(proj, pair, heads, 2)
                for i in range(heads):
                    v_s[i] = pick(v, i, width)

    def att_copy(g, t, to):
        i = lax.rem(me + 1 + t, per)
        j = g // seqs
        return rcopy(
            att_s.at[g, pl.ds(pl.multiple_of(i * share, share), share)],
            att_all.at[me, j],
            a_send.at[g, t],
            a_recv.at[j, me],
            (row, to),
        )

    def att_keep(g, t):
        i = lax.rem(me + 1 + t, per)
        return pltpu.make_async_copy(
            att_s.at[g, pl.ds(pl.multiple_of(i * share, share), share)], att_all.at[me, g // seqs], l_sem.at[3]
        )

    def att_to(g, t):
        return lax.rem(g, seqs) * per + lax.rem(me + 1 + t, per)

    def att_send(done):
        g = done // turns
        t = lax.rem(done, turns) // in_share
        to = att_to(g, t)

        @pl.when(to != me)
        def _():
            att_copy(g, t, to).start()

        @pl.when(to == me)
        def _():
            c = att_keep(g, t)
            c.start()
            c.wait()

    @pl.when((step > 0) & (lax.rem(step, in_share) == 0))
    def _():
        att_send(step - 1)

    at_step = {1: [(0, 2)], 2: [(1, 2)], 4: [(0, 3)], 5: [(1, 3)], 7: [(0, 4), (1, 4)]}
    for h in range(5, far + 1):
        at_step[7] += [(0, h), (1, h)]
    for n, todo in at_step.items():

        @pl.when(step == n * steps // 8)
        def _(todo=todo):
            for k, h in todo:
                handle(k, h)

    @pl.when(step == 1)
    def _():
        for c in saves():
            c.start()

    rows_now = pl.ds(pl.multiple_of(turn * block, block), block)
    raws, probs, out = forward_block(
        q_s[rows_now, :], k_s[...], [v_s[i] for i in range(heads)], [prev[i] for i in range(heads)], width
    )
    for i in range(heads):
        raw[i] = raws[i]
        prob[i] = probs[i]
    att_s[group, rows_now, :] = out.astype(BF16)

    @pl.when(step == steps - 1)
    def _():
        att_send(step)
        for c in saves():
            c.wait()
        for j in offs:
            for kind in kinds:
                x_copy(kind, j).wait_send()
                if kind in ("vec", "og"):
                    x_got(kind, j).wait_recv()
        for way in range(2):
            for h in range(1, depth(chips, 0, way) + 1):
                q_hop(way, h).wait_send()
            for h in range(0 if way == 0 else 1, depth(chips, 0, way) + 1):
                q_pair(way, h).wait_send()
            for k in range(2):
                for p in range(len(pieces)):
                    for h in range(1, depth(chips, k, way) + 1):
                        f_hop(k, p, way, h).wait_send()
                    for h in range(0 if way == 0 else 1, depth(chips, k, way) + 1):
                        f_pair(k, p, way, h).wait_send()
                        f_pair(k, p, way, h, mine=False).wait_recv()
        keep = pltpu.make_async_copy(wf_v, wf_all, l_sem.at[4])
        keep.start()
        for g in range(pairs * seqs):
            for t in range(per):
                to = att_to(g, t)

                @pl.when(to != me)
                def _():
                    att_copy(g, t, to).wait_send()

        for p in range(pairs):
            for j in offs:
                came = at.peer(j)
                rcopy(
                    att_s.at[0, pl.ds(0, share)], att_all.at[came, p], a_send.at[0, 0], a_recv.at[p, came], at.col_peer(j)
                ).wait_recv()
        keep.wait()


def front(cols, rows_dev, seqs, head_count, tok, wq, w_out, w_ff1, w_ff2, sides, og, bias, prev):
    heads = min(2, head_count)
    pairs = head_count // heads
    total, feat = tok.shape
    share = total // cols
    length = prev.shape[-1]
    width = heads * DH
    block = min(256, share)
    turns = length // block
    per = length // share
    in_share = share // block
    chips = rows_dev // 2
    far = chips // 2
    groups = pairs * seqs
    shard = wq.shape[0]
    weights = w_out.shape[1] + 2 * w_ff1.shape[1]
    n = len(cuts(weights))

    def stream(s):
        g = s // turns
        turn = lax.rem(lax.rem(s, turns) + lax.rem(lax.axis_index("col") + 1, per) * in_share, turns)
        return (lax.rem(g, seqs) * pairs + g // seqs, turn, 0)

    def whole(x):
        n = x.ndim
        return pl.BlockSpec(x.shape, lambda s: (0,) * n, pipeline_mode=pl.Buffered(1))

    blocks = pl.BlockSpec((heads, block, length), stream)
    anywhere = pl.BlockSpec(memory_space=pl.ANY)
    dma = pltpu.SemaphoreType.DMA
    shapes = [
        (cols, total, feat),
        (total, wq.shape[1]),
        (rows_dev, cols, shard, weights),
        (rows_dev,) + wq.shape,
        (cols, 16, feat),
        (cols, share, feat),
        (cols, pairs, share, width),
    ]
    return pl.pallas_call(
        functools.partial(front_kernel, (cols, rows_dev, seqs, heads, pairs, share, block)),
        grid=(groups * turns,),
        in_specs=[whole(x) for x in (tok, wq, w_out, w_ff1, w_ff2, *sides, og, bias)] + [blocks],
        out_specs=[blocks, blocks] + [anywhere] * 7,
        out_shape=[jax.ShapeDtypeStruct(prev.shape, BF16)] * 2 + [jax.ShapeDtypeStruct(s, BF16) for s in shapes],
        scratch_shapes=[
            pltpu.VMEM((cols, total, feat), BF16),
            pltpu.VMEM((rows_dev,) + wq.shape, BF16),
            pltpu.VMEM((total, wq.shape[1]), BF16),
            pltpu.VMEM((length, width), BF16),
            pltpu.VMEM((length, width), BF16),
            pltpu.VMEM((heads, length, width), BF16),
            pltpu.VMEM((groups, length, width), BF16),
            pltpu.VMEM((shard, weights), BF16),
            pltpu.VMEM((16, feat), BF16),
            pltpu.VMEM((rows_dev, cols, shard, weights), BF16),
            dma((5, cols - 1)),
            dma((5, cols - 1)),
            dma((4, far + 1)),
            dma((4, far + 1)),
            dma((2, n, 2, far)),
            dma((2, n, 2, far)),
            dma((2, n, 2, far + 1)),
            dma((2, n, 2, far + 1)),
            dma((groups, per)),
            dma((pairs, cols)),
            dma((5,)),
        ],
        compiler_params=pltpu.CompilerParams(
            collective_id=1, has_side_effects=True, vmem_limit_bytes=60 << 20
        ),
        name="front",
    )(tok, wq, w_out, w_ff1, w_ff2, *sides, og, bias, prev)


def back_kernel(
    dims, proj, wq, tok, datt, outp, dh, gvec, gw, prob, cot,
    pg, out_all, ig, gwo, gqo, gvo,
    datt_s, out_s, dh_s, q_s, k_s, v_s, dq_s, dk_s, dv_s, dp_s,
    own_s, part_s, run_s, run_r, fin_s, fin_r,
    gq_s, gq_p, gq_t, gq_r, ip_s, xi_s, xi_r, vp_s, vs_s, vx_s, vr_s,
    x_send, x_recv, p_send, p_recv, r_send, r_recv, g_send, g_recv, v_send, v_recv, l_sem,
):
    cols, rows_dev, seqs, heads, pairs, share, block = dims
    at = Spot(rows_dev, cols)
    chips, me, core = at.chips, at.me, at.core
    chip = at.row // 2
    half_size = cols // 2
    width = heads * DH
    wide = 3 * width
    length = prob.shape[2]
    per = length // share
    turns = length // block
    in_share = share // block
    shard = gw.shape[3]
    pieces = cuts(gw.shape[4])
    step = pl.program_id(0)
    steps = pairs * seqs * turns
    group = step // turns
    pos = lax.rem(step, turns)
    pair_now = group // seqs
    seq_now = lax.rem(group, seqs)
    turn = lax.rem(pos + lax.rem(me, per) * in_share, turns)
    offs = list(range(1, cols))
    hops = list(range(1, chips))
    far = chips // 2
    total_rows = seqs * length

    def half(k):
        mine = me // half_size
        first = mine if k == 0 else 1 - mine
        return pl.ds(first * half_size, half_size)

    def chip_of(o):
        return chip_at(at.place + o, chips)

    def to_chip(o):
        return (2 * chip_of(o) + core, me)

    def x_copy(kind, j):
        to = at.peer(j)
        src, dst = [
            lambda: (datt.at[to], datt_s.at[me]),
            lambda: (outp.at[to], out_s.at[me]),
            lambda: (dh.at[to], dh_s.at[me]),
            lambda: (fin_s.at[to], fin_r.at[me]),
            lambda: (xi_s.at[j - 1], xi_r.at[j - 1]),
            lambda: (vs_s.at[to], vx_s.at[me]),
        ][kind]()
        return rcopy(src, dst, x_send.at[kind, j - 1], x_recv.at[kind, j - 1], at.col_peer(j))

    def x_got(kind, j):
        came = at.peer(-j)
        src, dst = [
            lambda: (datt.at[came], datt_s.at[came]),
            lambda: (outp.at[came], out_s.at[came]),
            lambda: (dh.at[came], dh_s.at[came]),
            lambda: (fin_s.at[came], fin_r.at[came]),
            lambda: (xi_s.at[j - 1], xi_r.at[j - 1]),
            lambda: (vs_s.at[came], vx_s.at[came]),
        ][kind]()
        return rcopy(src, dst, x_send.at[kind, j - 1], x_recv.at[kind, j - 1], at.col_peer(j))

    def part_copy(o):
        c = chip_of(o)
        return rcopy(gw.at[c, 1 - core], part_s.at[c], p_send.at[o % chips], p_recv.at[o % chips], at.partner)

    def own_load():
        return pltpu.make_async_copy(gw.at[:, core], own_s, l_sem.at[0])

    def locals_():
        return [
            pltpu.make_async_copy(datt.at[me], datt_s.at[me], l_sem.at[1]),
            pltpu.make_async_copy(outp.at[me], out_s.at[me], l_sem.at[2]),
            pltpu.make_async_copy(dh.at[me], dh_s.at[me], l_sem.at[3]),
        ]

    def run_copy(k, p, way, t):
        here = (k, p, way, t - 1)
        return rcopy(run_s.at[here], run_r.at[here], r_send.at[here], r_recv.at[here], at.ring(way))

    waited = set()

    def chip_sum(k, p, o):
        if o % chips not in waited:
            waited.add(o % chips)
            part_copy(o).wait_recv()
        c = chip_of(o)
        return own_s[c, half(k), :, pieces[p]].astype(F32) + part_s[c, half(k), :, pieces[p]].astype(F32)

    def run_step(k, p, t):
        for way in range(2):
            o = depth(chips, k, way) + 1 - t
            if o < 1:
                continue
            value = chip_sum(k, p, o if way == 0 else -o)
            if t > 1:
                run_copy(k, p, way, t - 1).wait_recv()
                value = value + run_r[k, p, way, t - 2].astype(F32)
            run_s[k, p, way, t - 1] = value.astype(BF16)
            run_copy(k, p, way, t).start()

    def run_last(k, p):
        value = chip_sum(k, p, 0)
        for way in range(2):
            d = depth(chips, k, way)
            run_copy(k, p, way, d).wait_recv()
            value = value + run_r[k, p, way, d - 1].astype(F32)
        fin_s[half(k), :, pieces[p]] = value.astype(BF16)

    streams = [(k, p) for p in range(len(pieces)) for k in range(2)]

    def run_round(t, only=None):
        for n, (k, p) in enumerate(streams):
            if only is None or n in only:
                run_step(k, p, t)

    def v_pair():
        return rcopy(gvec, vp_s, v_send.at[0], v_recv.at[0], at.partner)

    def v_chip(o):
        return rcopy(vr_s.at[chip], vr_s.at[chip], v_send.at[o], v_recv.at[o], to_chip(o))

    def v_chip_got(o):
        c = chip_of(-o)
        return rcopy(vr_s.at[c], vr_s.at[c], v_send.at[o], v_recv.at[o], to_chip(o))

    def v_second():
        v_pair().wait_recv()
        vs_s[...] = gvec[...] + vp_s[...]
        for j in offs:
            x_copy(5, j).start()

    def v_third():
        value = vs_s[me]
        for j in offs:
            x_got(5, j).wait_recv()
            value = value + vx_s[at.peer(-j)]
        vr_s[chip] = value
        for o in hops:
            v_chip(o).start()

    def g_pair(j):
        return rcopy(gq_s.at[:, 1 - core], gq_p.at[j], g_send.at[j, 0], g_recv.at[j, 0], at.partner)

    def g_chip(j, o):
        return rcopy(gq_t.at[j, chip_of(o)], gq_r.at[j, chip], g_send.at[j, o], g_recv.at[j, o], to_chip(o))

    def g_chip_got(j, o):
        return rcopy(gq_t.at[j, 0], gq_r.at[j, chip_of(-o)], g_send.at[j, o], g_recv.at[j, o], to_chip(o))

    def g_weight(j):
        slots = chips // cols
        for c in range(cols):
            value = dot_tn(tok[c], dp_s[...]).astype(BF16)
            gq_s[c * slots : (c + 1) * slots, :, :shard, :] = value.reshape(slots, 2, shard, wide)
        sums = col_sum(dp_s[...].astype(F32))
        line = lax.broadcasted_iota(jnp.int32, (16, wide), 0)
        low = jnp.where(line == 0, jnp.broadcast_to(sums, (16, wide)), 0.0).astype(BF16)
        gq_s[:, :, shard:, :] = jnp.broadcast_to(low[None, None], (chips, 2, 16, wide))
        g_pair(j).start()

    def g_pass(j):
        g_pair(j).wait_recv()
        gq_t[j] = (gq_s[:, core].astype(F32) + gq_p[j].astype(F32)).astype(BF16)
        gq_r[j, chip] = gq_t[j, chip]
        for o in hops:
            g_chip(j, o).start()

    def g_last(j):
        for o in hops:
            g_chip_got(j, o).wait_recv()
        value = gq_r[j, 0].astype(F32)
        for c in range(1, chips):
            value = value + gq_r[j, c].astype(F32)
        gqo[:, j * wide : (j + 1) * wide] = value

    chunk = min(512, total_rows)

    def input_part(j, n):
        slots = rows_dev // cols
        w = wq[pl.ds(at.peer(n) * slots, slots), :, j * wide : (j + 1) * wide].reshape(slots * shard, wide)

        def go(i, carry):
            span = pl.ds(pl.multiple_of(i * chunk, chunk), chunk)
            value = dot_nt(dp_s[span, :], w)
            if j > 0:
                value = value + ip_s[n, span, :]
            if j < pairs - 1:
                ip_s[n, span, :] = value
            elif n > 0:
                xi_s[n - 1, span, :] = value.astype(BF16)
            else:
                ip_s[0, span, :] = value
            return carry

        lax.fori_loop(0, total_rows // chunk, go, 0)

    @pl.when(step == 0)
    def _():
        greet(
            [at.ring(0), at.ring(1), at.partner]
            + [at.col_peer(j) for j in offs]
            + [to_chip(o) for o in hops if o not in (1, chips - 1)]
        )
        for j in offs:
            x_copy(0, j).start()
        own_load().start()
        v_pair().start()
        order = [far] + [s * o for o in range(far - 1, 0, -1) for s in (1, -1)] + [0]
        for o in order:
            part_copy(o).start()
        for c in locals_():
            c.start()
        for c in locals_():
            c.wait()
        if seqs > 1:
            for j in offs:
                x_got(0, j).wait_recv()

    if seqs == 1:

        @pl.when(step == in_share)
        def _():
            for j in offs:
                x_got(0, j).wait_recv()

    @pl.when(pos == 0)
    def _():
        for pair in range(pairs):

            @pl.when(pair_now == pair)
            def _():
                here = proj[pl.ds(pl.multiple_of(seq_now * length, length), length), :]
                q_s[...] = part_of(here, pair, heads, 0) * jnp.asarray(0.125, BF16)
                k = part_of(here, pair, heads, 1)
                for i in range(heads):
                    k_s[i] = pick(k, i, width)
                v_s[...] = part_of(here, pair, heads, 2)

        dk_s[...] = jnp.zeros_like(dk_s)
        dv_s[...] = jnp.zeros_like(dv_s)

    jobs = {
        0: [lambda: own_load().wait(), lambda: run_round(1)],
        1: [v_second, *[lambda kind=kind, j=j: x_copy(kind, j).start() for kind in (1, 2) for j in offs]],
        3: [v_third, lambda: run_round(2, (0,))],
        4: [lambda: run_round(2, (1, 2))],
        5: [lambda: run_round(2, (3,))],
        7: [lambda: run_round(3, (0, 1))],
    }

    def spot(n):
        return (n * steps) // 8

    for n, todo in jobs.items():

        @pl.when(step == spot(n))
        def _(todo=todo):
            for job in todo:
                job()

    @pl.when((step == steps // pairs) & (pairs > 1))
    def _():
        if pairs > 1:
            g_pass(0)

    rows_now = pl.ds(pl.multiple_of(turn * block, block), block)
    q_rows = q_s[rows_now, :]
    source = seq_now * per + turn // in_share
    inside = pl.ds(pl.multiple_of(lax.rem(turn, in_share) * block, block), block)
    dq = dk = dv = None
    for pair in range(pairs):

        @pl.when(pair_now == pair)
        def _():
            dq = dk = dv = None
            d_rows = datt_s[source, inside, pair * width : (pair + 1) * width]
            for i in range(heads):
                d_one = pick(d_rows, i, width)
                d_probs = dot_nt(d_one, v_s[...])
                p = prob[i]
                p_wide = p.astype(F32)
                delta = jnp.sum(d_probs * p_wide, axis=1, keepdims=True)
                low = (p_wide * (d_probs - delta) + cot[i].astype(F32)).astype(BF16)
                pg[i] = low
                a = dot_nn(low, k_s[i])
                b = dot_tn(pick(q_rows, i, width), low)
                c = dot_tn(d_one, p)
                dq = a if dq is None else dq + a
                dk = b if dk is None else dk + b
                dv = c if dv is None else dv + c
            dq_s[rows_now, :] = (dq * 0.125).astype(BF16)
            dk_s[...] += dk
            dv_s[...] += dv

    @pl.when(pos == turns - 1)
    def _():
        parts = [dq_s[...], dk_s[...].T.astype(BF16), dv_s[...].T.astype(BF16)]
        here = pl.ds(pl.multiple_of(seq_now * length, length), length)
        for i in range(heads):
            dp_s[here, i * 3 * DH : (i + 1) * 3 * DH] = jnp.concatenate([p[:, i * DH : (i + 1) * DH] for p in parts], axis=1)

    for j in range(pairs - 1):

        @pl.when(step == (j + 1) * (steps // pairs) - 1)
        def _():
            g_weight(j)
            for n in range(cols):
                input_part(j, n)

    @pl.when(step == steps - 1)
    def _():
        last = pairs - 1
        for j in offs:
            input_part(last, j)
            x_copy(4, j).start()
        if pairs > 1:
            g_pair(last - 1).wait_send()
        run_round(3, (2, 3))
        run_round(4)
        g_weight(last)
        for t in range(5, far + 1):
            run_round(t)
        input_part(last, 0)
        g_pass(last)
        for j in offs:
            x_got(1, j).wait_recv()
            x_got(2, j).wait_recv()
        keep = pltpu.make_async_copy(out_s, out_all, l_sem.at[1])
        keep.start()
        for k, p in streams:
            run_last(k, p)
        for j in offs:
            x_copy(3, j).start()
        for o in hops:
            v_chip_got(o).wait_recv()
        value = vr_s[0]
        for c in range(1, chips):
            value = value + vr_s[c]
        gvo[...] = value
        for j in range(pairs):
            g_last(j)
        for j in offs:
            x_got(4, j).wait_recv()

        def finish(i, carry):
            c = i // (share // min(share, chunk))
            rows = min(share, chunk)
            inner = pl.ds(pl.multiple_of(lax.rem(i, share // rows) * rows, rows), rows)
            span = pl.ds(pl.multiple_of(i * rows, rows), rows)
            value = ip_s[0, span, :] + dh_s[c, inner, :].astype(F32)
            for j in offs:
                value = value + xi_r[j - 1, span, :].astype(F32)
            ig[span, :] = value.astype(BF16)
            return carry

        lax.fori_loop(0, total_rows // min(share, chunk), finish, 0)
        value = fin_s[me].astype(F32)
        for j in offs:
            x_got(3, j).wait_recv()
            value = value + fin_r[at.peer(-j)].astype(F32)
        gwo[...] = value
        keep.wait()
        for kind in range(6):
            for j in offs:
                x_copy(kind, j).wait_send()
        for o in range(chips):
            part_copy(o).wait_send()
        for k in range(2):
            for way in range(2):
                for t in range(1, depth(chips, k, way) + 1):
                    for p in range(len(pieces)):
                        run_copy(k, p, way, t).wait_send()
        v_pair().wait_send()
        for o in hops:
            v_chip(o).wait_send()
        g_pair(last).wait_send()
        for j in range(pairs):
            for o in hops:
                g_chip(j, o).wait_send()


def back(cols, rows_dev, seqs, head_count, proj, wq, tok, datt, outp, dh, gvec, gw, prob, cot):
    heads = min(2, head_count)
    pairs = head_count // heads
    _, total, feat = tok.shape
    share = total // cols
    length = prob.shape[-1]
    width = heads * DH
    wide = 3 * width
    block = min(256, share)
    turns = length // block
    per = length // share
    in_share = share // block
    chips = rows_dev // 2
    far = chips // 2
    shard, weights = gw.shape[2:]
    half_size = cols // 2
    n = len(cuts(weights))
    gw = gw.reshape(chips, 2, cols, shard, weights)

    def stream(s):
        g = s // turns
        turn = lax.rem(lax.rem(s, turns) + lax.rem(lax.axis_index("col"), per) * in_share, turns)
        return (lax.rem(g, seqs) * pairs + g // seqs, turn, 0)

    def whole(shape):
        n = len(shape)
        return pl.BlockSpec(shape, lambda s: (0,) * n, pipeline_mode=pl.Buffered(1))

    blocks = pl.BlockSpec((heads, block, length), stream)
    anywhere = pl.BlockSpec(memory_space=pl.ANY)
    dma = pltpu.SemaphoreType.DMA
    outs = [
        jax.ShapeDtypeStruct(prob.shape, BF16),
        jax.ShapeDtypeStruct((cols, share, feat), BF16),
        jax.ShapeDtypeStruct((total, feat), BF16),
        jax.ShapeDtypeStruct((shard, weights), F32),
        jax.ShapeDtypeStruct((shard + 16, wq.shape[2]), F32),
        jax.ShapeDtypeStruct(gvec.shape[1:], F32),
    ]
    return pl.pallas_call(
        functools.partial(back_kernel, (cols, rows_dev, seqs, heads, pairs, share, block)),
        grid=(pairs * seqs * turns,),
        in_specs=[whole(x.shape) for x in (proj, wq, tok, datt, outp, dh, gvec)] + [anywhere, blocks, blocks],
        out_specs=[blocks, anywhere] + [whole(o.shape) for o in outs[2:]],
        out_shape=outs,
        scratch_shapes=[
            pltpu.VMEM(datt.shape, BF16),
            pltpu.VMEM(outp.shape, BF16),
            pltpu.VMEM(dh.shape, BF16),
            pltpu.VMEM((length, width), BF16),
            pltpu.VMEM((heads, length, width), BF16),
            pltpu.VMEM((length, width), BF16),
            pltpu.VMEM((length, width), BF16),
            pltpu.VMEM((width, length), F32),
            pltpu.VMEM((width, length), F32),
            pltpu.VMEM((total, wide), BF16),
            pltpu.VMEM((chips, cols, shard, weights), BF16),
            pltpu.VMEM((chips, cols, shard, weights), BF16),
            pltpu.VMEM((2, n, 2, far, half_size, shard, weights // n), BF16),
            pltpu.VMEM((2, n, 2, far, half_size, shard, weights // n), BF16),
            pltpu.VMEM((cols, shard, weights), BF16),
            pltpu.VMEM((cols, shard, weights), BF16),
            pltpu.VMEM((chips, 2, shard + 16, wide), BF16),
            pltpu.VMEM((pairs, chips, shard + 16, wide), BF16),
            pltpu.VMEM((pairs, chips, shard + 16, wide), BF16),
            pltpu.VMEM((pairs, chips, shard + 16, wide), BF16),
            pltpu.VMEM((cols if pairs > 1 else 1, total, feat), F32),
            pltpu.VMEM((cols - 1, total, feat), BF16),
            pltpu.VMEM((cols - 1, total, feat), BF16),
            pltpu.VMEM(gvec.shape, F32),
            pltpu.VMEM(gvec.shape, F32),
            pltpu.VMEM(gvec.shape, F32),
            pltpu.VMEM((chips,) + gvec.shape[1:], F32),
            dma((6, cols - 1)),
            dma((6, cols - 1)),
            dma((chips,)),
            dma((chips,)),
            dma((2, n, 2, far)),
            dma((2, n, 2, far)),
            dma((pairs, chips)),
            dma((pairs, chips)),
            dma((chips,)),
            dma((chips,)),
            dma((4,)),
        ],
        compiler_params=pltpu.CompilerParams(
            collective_id=2, has_side_effects=True, vmem_limit_bytes=62 << 20
        ),
        name="back",
    )(proj, wq, tok, datt, outp, dh, gvec, gw, prob, cot)


def finish_kernel(
    pg_in, out_in, ig_in, gw, gq, gv, pg, out, ig, wq, bq, wo, bo, n1g, n1s, w1, b1, w2, b2, n2g, n2s,
    bounce, out_s, ig_s, in_sem, out_sem,
):
    ways = [(pg_in.at[n], bounce.at[n], pg.at[n]) for n in range(bounce.shape[0])]
    ways += [(out_in, out_s, out), (ig_in, ig_s, ig)]
    slots = len(ways)
    takes = [pltpu.make_async_copy(a, b, in_sem.at[n]) for n, (a, b, _) in enumerate(ways)]
    puts = [pltpu.make_async_copy(b, c, out_sem.at[n]) for n, (_, b, c) in enumerate(ways)]
    for c in takes:
        c.start()
    shard = wq.shape[0]
    hw, fw = wo.shape[1], w1.shape[1]
    feat = gv.shape[1]
    for n in range(slots // 2):
        takes[n].wait()
        puts[n].start()
    wq[...] = gq[:shard]
    bq[...] = gq[shard : shard + 1].reshape(-1)
    wo[...] = gw[:, :hw]
    w1[...] = gw[:, hw : hw + fw]
    w2[...] = gw[:, hw + fw :]
    for i, ref in enumerate((bo, n1g, n1s, b2, n2g, n2s)):
        ref[...] = gv[i : i + 1].reshape(-1)
    b1[...] = jnp.concatenate([gv[6 + i : 7 + i] for i in range(fw // feat)], axis=1).reshape(-1)
    for n in range(slots // 2, slots):
        takes[n].wait()
        puts[n].start()
    for c in puts:
        c.wait()


def finish(pg, out, ig, gw, gq, gv, hw, fw):
    slots = 4
    pieces = (slots, pg.shape[0] * pg.shape[1] // slots, pg.shape[2])
    total, feat = ig.shape
    shard = gw.shape[0]
    vmem = pl.BlockSpec(memory_space=pltpu.VMEM)
    anywhere = pl.BlockSpec(memory_space=pl.ANY)

    def f32(*shape):
        return jax.ShapeDtypeStruct(shape, F32)

    outs = [
        jax.ShapeDtypeStruct(pieces, BF16),
        jax.ShapeDtypeStruct(ig.shape, BF16),
        jax.ShapeDtypeStruct(ig.shape, BF16),
        f32(shard, gq.shape[1]),
        f32(gq.shape[1]),
        f32(shard, hw),
        f32(feat),
        f32(feat),
        f32(feat),
        f32(shard, fw),
        f32(fw),
        f32(shard, fw),
        f32(feat),
        f32(feat),
        f32(feat),
    ]
    return pl.pallas_call(
        finish_kernel,
        out_shape=outs,
        in_specs=[anywhere] * 3 + [vmem] * 3,
        out_specs=[anywhere] * 3 + [vmem] * 12,
        scratch_shapes=[
            pltpu.VMEM(pieces, BF16),
            pltpu.VMEM(ig.shape, BF16),
            pltpu.VMEM(ig.shape, BF16),
            pltpu.SemaphoreType.DMA((slots + 2,)),
            pltpu.SemaphoreType.DMA((slots + 2,)),
        ],
        compiler_params=pltpu.CompilerParams(vmem_limit_bytes=60 << 20),
        name="finish",
    )(pg.reshape(pieces), out.reshape(ig.shape), ig, gw, gq, gv)


def per_device(
    cols,
    row_count,
    tokens,
    prev_logits,
    qkv_weight,
    qkv_bias,
    out_weight,
    out_bias,
    norm1_gain,
    norm1_shift,
    ff1_weight,
    ff1_bias,
    ff2_weight,
    ff2_bias,
    norm2_gain,
    norm2_shift,
    out_grad,
    logit_grad,
):
    seqs, head_count, length, _ = prev_logits.shape
    total, feat = tokens.shape
    share = total // cols
    rows = min(256, length)
    rows_dev = row_count
    hidden = ff1_weight.shape[1]
    sides = (out_bias, norm1_gain, norm1_shift, ff2_bias, norm2_gain, norm2_shift, ff1_bias)
    prev = prev_logits.reshape(seqs * head_count, length, length)
    cot = logit_grad.reshape(seqs * head_count, length, length)
    raw, prob, tok_all, proj, wf_all, wq_all, vec_all, og_all, att_all = front(
        cols, rows_dev, seqs, head_count, tokens, qkv_weight, out_weight.T, ff1_weight, ff2_weight.T, sides, out_grad, qkv_bias, prev
    )
    out, dh, datt, gvec, gw, raw = middle(tok_all, att_all, og_all, wf_all, vec_all, raw)

    prev_grad, output, input_grad, gw, gq, gv = back(
        cols, rows_dev, seqs, head_count, proj, wq_all, tok_all, datt, out, dh, gvec, gw, prob, cot
    )
    prev_grad, output, input_grad, *rest = finish(
        prev_grad, output, input_grad, gw, gq, gv, out_weight.shape[0], hidden
    )
    rest[2] = rest[2].T
    rest[8] = rest[8].T
    return output, raw.reshape(prev_logits.shape), input_grad, prev_grad.reshape(prev_logits.shape), *rest


def solution(mesh):
    in_specs = (
        P("row", "col"),
        P("row", "col", None, None),
        P("row", "col"),
        P("col"),
        P("col", "row"),
        P("col"),
        P("col"),
        P("col"),
        P("row", "col"),
        P("col"),
        P("col", "row"),
        P("col"),
        P("col"),
        P("col"),
        P("row", "col"),
        P("row", "col", None, None),
    )
    out_specs = (
        P("row", "col"),
        P("row", "col", None, None),
        P("row", "col"),
        P("row", "col", None, None),
        P("row", "col"),
        P("col"),
        P("col", "row"),
        P("col"),
        P("col"),
        P("col"),
        P("row", "col"),
        P("col"),
        P("col", "row"),
        P("col"),
        P("col"),
        P("col"),
    )
    return jax.shard_map(
        functools.partial(per_device, mesh.shape["col"], mesh.shape["row"]),
        mesh=mesh,
        in_specs=in_specs,
        out_specs=out_specs,
        check_vma=False,
    )
```

```python
import functools
import math

import jax
import jax.numpy as jnp
from jax import lax
from jax.experimental import pallas as pl
from jax.experimental.pallas import tpu as pltpu
from jax.sharding import PartitionSpec as P

DH = 64
F32 = jnp.float32
BF16 = jnp.bfloat16
norm_eps = 1e-06
root_half = 0.7071067811865476
inv_root_two_pi = 0.3989422804014327
NT = (((1,), (1,)), ((), ()))
TN = (((0,), (0,)), ((), ()))


def dot_nn(a, b):
    return jnp.dot(a, b, preferred_element_type=F32)


def dot_nt(a, b):
    return lax.dot_general(a, b, NT, preferred_element_type=F32)


def dot_tn(a, b):
    return lax.dot_general(a, b, TN, preferred_element_type=F32)


def pick(value, index, width):
    if width == DH:
        return value
    lane = lax.broadcasted_iota(jnp.int32, value.shape, 1)
    keep = (lane >= index * DH) & (lane < (index + 1) * DH)
    return jnp.where(keep, value, jnp.zeros_like(value))


def part_of(proj, pair, heads, part):
    pieces = [
        proj[:, (pair * heads + i) * 3 * DH + part * DH :][:, :DH] for i in range(heads)
    ]
    return pieces[0] if heads == 1 else jnp.concatenate(pieces, axis=1)


def forward_block(q_rows, k_all, v_masked, prev, width):
    raws, probs, total = [], [], None
    for i in range(width // DH):
        scores = dot_nt(pick(q_rows, i, width), k_all) + prev[i].astype(F32)
        raws.append(scores.astype(BF16))
        exponent = jnp.exp(scores - jnp.max(scores, axis=1, keepdims=True))
        scale = 1.0 / jnp.sum(exponent, axis=1, keepdims=True)
        prob = (exponent * scale).astype(BF16)
        probs.append(prob)
        out = dot_nn(prob, v_masked[i])
        total = out if total is None else total + out
    return raws, probs, total


def normalize(hidden):
    width = hidden.shape[1]
    center = hidden - jnp.sum(hidden, axis=1, keepdims=True) * (1.0 / width)
    inv_std = lax.rsqrt(jnp.sum(center * center, axis=1, keepdims=True) * (1.0 / width) + norm_eps)
    return center * inv_std, inv_std


def norm_back(scaled, xhat, inv_std):
    width = scaled.shape[1]
    mean_grad = jnp.sum(scaled, axis=1, keepdims=True) * (1.0 / width)
    mean_cross = jnp.sum(scaled * xhat, axis=1, keepdims=True) * (1.0 / width)
    return inv_std * (scaled - mean_grad - xhat * mean_cross)


def col_sum(value):
    return jnp.sum(value, axis=0, keepdims=True)


def middle_kernel(
    dims, tok_ref, att_ref, og_ref, vec_ref, w_in, raw_in,
    out_ref, dh_ref, datt_ref, gvec_ref, gw_out, raw_out,
    act_s, slope_s, w_ref, gw_ref, bounce, w_sem, g_sem, in_sem, out_sem,
):
    cols, share, hw, fw = dims
    feat = vec_ref.shape[2]
    pairs, width = att_ref.shape[1], att_ref.shape[3]
    slots, rows_dev = bounce.shape[0], w_ref.shape[0]
    shard = w_ref.shape[2]
    cut = min(512, fw)
    me = lax.axis_index("col")

    total = w_ref.shape[3]
    ranges = [(0, hw), (hw, fw), (hw + fw, fw)] if hw % 128 == 0 and fw % 128 == 0 else [(0, total)]

    def columns(ref, n):
        return ref.at[:, :, :, pl.ds(*ranges[n])]

    loads = [pltpu.make_async_copy(columns(w_in, n), columns(w_ref, n), w_sem.at[n]) for n in range(len(ranges))]
    stores = [pltpu.make_async_copy(columns(gw_ref, n), columns(gw_out, n), g_sem.at[n]) for n in range(len(ranges))]
    split = len(ranges) == 3
    for c in loads:
        c.start()
    loads[0].wait()
    takes = [pltpu.make_async_copy(raw_in.at[n], bounce.at[n], in_sem.at[n]) for n in range(slots)]
    puts = [pltpu.make_async_copy(bounce.at[n], raw_out.at[n], out_sem.at[n]) for n in range(slots)]
    for c in takes:
        c.start()

    def side(ref, i):
        return jnp.concatenate([ref[c, i : i + 1] for c in range(cols)], axis=1).astype(F32)

    def weight(c, a, b):
        return w_ref[:, c, :, a:b].reshape(rows_dev * shard, b - a)

    def put_weight(c, a, b, value):
        gw_ref[:, c, :, a:b] = value.astype(BF16).reshape(rows_dev, shard, b - a)

    own = pl.ds(pl.multiple_of(me * share, share), share)
    out_bias, gain1, shift1, ff2_bias, gain2, shift2 = (side(vec_ref, i) for i in range(6))
    tok = jnp.concatenate([tok_ref[c, own, :] for c in range(cols)], axis=1)

    hidden1 = tok.astype(F32) + out_bias
    for c in range(cols):
        for j in range(pairs):
            hidden1 = hidden1 + dot_nt(att_ref[c, j], weight(c, j * width, (j + 1) * width))
    xhat1, inv1 = normalize(hidden1)
    normed1 = xhat1 * gain1 + shift1
    low1 = normed1.astype(BF16)

    chunks = [(c, o) for c in range(cols) for o in range(0, fw, cut)]
    hidden2 = normed1 + ff2_bias
    if split:
        loads[1].wait()
        loads[2].wait()
    for c, o in chunks:
        at = c * fw + o
        bias = jnp.concatenate([vec_ref[c, 6 + (o + i) // feat : 7 + (o + i) // feat] for i in range(0, cut, feat)], axis=1)
        inner = dot_nn(low1, weight(c, hw + o, hw + o + cut)) + bias.astype(F32)
        half = 0.5 + 0.5 * lax.erf(inner * root_half)
        act = (inner * half).astype(BF16)
        act_s[:, at : at + cut] = act
        slope_s[:, at : at + cut] = half + inner * inv_root_two_pi * jnp.exp(-0.5 * inner * inner)
        hidden2 = hidden2 + dot_nt(act, weight(c, hw + fw + o, hw + fw + o + cut))
    for n in range(slots):
        takes[n].wait()
        puts[n].start()
    xhat2, inv2 = normalize(hidden2)
    output = (xhat2 * gain2 + shift2).astype(BF16)

    og = jnp.concatenate([og_ref[c] for c in range(cols)], axis=1).astype(F32)
    d_hidden2 = norm_back(og * gain2, xhat2, inv2)
    low2 = d_hidden2.astype(BF16)
    rows = [None] * 6
    rows[4] = col_sum(og * xhat2)
    rows[5] = col_sum(og)
    rows[3] = col_sum(low2.astype(F32))
    low1_t = low1.T
    low2_t = low2.T
    d_normed1 = d_hidden2
    for c, o in chunks:
        at = c * fw + o
        d_act = dot_nn(low2, weight(c, hw + fw + o, hw + fw + o + cut))
        d_inner = (d_act * slope_s[:, at : at + cut]).astype(BF16)
        d_normed1 = d_normed1 + dot_nt(d_inner, weight(c, hw + o, hw + o + cut))
        put_weight(c, hw + o, hw + o + cut, dot_nn(low1_t, d_inner))
        put_weight(c, hw + fw + o, hw + fw + o + cut, dot_nn(low2_t, act_s[:, at : at + cut]))
        sums = col_sum(d_inner.astype(F32))
        for i in range(0, cut, feat):
            gvec_ref[c, 6 + (o + i) // feat : 7 + (o + i) // feat] = sums[:, i : i + feat]

    if split:
        stores[1].start()
        stores[2].start()
    rows[1] = col_sum(d_normed1 * xhat1)
    rows[2] = col_sum(d_normed1)
    d_hidden1 = norm_back(d_normed1 * gain1, xhat1, inv1)
    low = d_hidden1.astype(BF16)
    rows[0] = col_sum(low.astype(F32))
    low_t = low.T
    spare = gvec_ref.shape[1] - 6 - fw // feat
    for c in range(cols):
        for j in range(pairs):
            put_weight(c, j * width, (j + 1) * width, dot_nn(low_t, att_ref[c, j]))
        datt_ref[c] = dot_nn(low, weight(c, 0, hw)).astype(BF16)
        span = slice(c * feat, (c + 1) * feat)
        out_ref[c] = output[:, span]
        dh_ref[c] = low[:, span]
        for i in range(6):
            gvec_ref[c, i : i + 1] = rows[i][:, span]
        if spare:
            gvec_ref[c, 6 + fw // feat :] = jnp.zeros((spare, feat), F32)
    stores[0].start()
    for c in puts:
        c.wait()
    for c in stores:
        c.wait()


def middle(tok, att, og, w, vec, raw):
    rows_dev, cols, shard, _ = w.shape
    feat = tok.shape[2]
    share = og.shape[1]
    hw = att.shape[1] * att.shape[3]
    fw = (w.shape[3] - hw) // 2
    slots = 4
    pieces = (slots, raw.shape[0] * raw.shape[1] // slots, raw.shape[2])
    vmem = pl.BlockSpec(memory_space=pltpu.VMEM)
    anywhere = pl.BlockSpec(memory_space=pl.ANY)
    results = pl.pallas_call(
        functools.partial(middle_kernel, (cols, share, hw, fw)),
        out_shape=[
            jax.ShapeDtypeStruct((cols, share, feat), BF16),
            jax.ShapeDtypeStruct((cols, share, feat), BF16),
            jax.ShapeDtypeStruct((cols, share, hw), BF16),
            jax.ShapeDtypeStruct(vec.shape, F32),
            jax.ShapeDtypeStruct(w.shape, BF16),
            jax.ShapeDtypeStruct(pieces, BF16),
        ],
        in_specs=[vmem] * 4 + [anywhere] * 2,
        out_specs=[vmem] * 4 + [anywhere] * 2,
        scratch_shapes=[
            pltpu.VMEM((share, cols * fw), BF16),
            pltpu.VMEM((share, cols * fw), F32),
            pltpu.VMEM(w.shape, BF16),
            pltpu.VMEM(w.shape, BF16),
            pltpu.VMEM(pieces, BF16),
            pltpu.SemaphoreType.DMA((3,)),
            pltpu.SemaphoreType.DMA((3,)),
            pltpu.SemaphoreType.DMA((slots,)),
            pltpu.SemaphoreType.DMA((slots,)),
        ],
        compiler_params=pltpu.CompilerParams(vmem_limit_bytes=60 << 20),
        name="middle",
    )(tok, att, og, vec, w, raw.reshape(pieces))
    return *results[:-1], results[-1].reshape(raw.shape)


MESH = pl.DeviceIdType.MESH


def chip_at(place, chips):
    place = lax.rem(place + 2 * chips, chips)
    return jnp.where(place < chips // 2, 2 * place, 2 * (chips - 1 - place) + 1)


def place_of(chip, chips):
    return jnp.where(lax.rem(chip, 2) == 0, chip // 2, chips - 1 - chip // 2)


class Spot:
    def __init__(self, devices_row, cols):
        self.cols = cols
        self.chips = devices_row // 2
        self.row = lax.axis_index("row")
        self.me = lax.axis_index("col")
        self.core = lax.rem(self.row, 2)
        self.place = place_of(self.row // 2, self.chips)
        self.partner = (self.row + 1 - 2 * self.core, self.me)

    def row_at(self, offset):
        return 2 * chip_at(self.place + offset, self.chips) + self.core

    def ring(self, way):
        return (self.row_at(1 if way == 0 else -1), self.me)

    def peer(self, j):
        return lax.rem(self.me + j + self.cols, self.cols)

    def col_peer(self, j):
        return (self.row, self.peer(j))


def greet(others):
    barrier = pltpu.get_barrier_semaphore()
    for other in others:
        pl.semaphore_signal(barrier, inc=1, device_id=other, device_id_type=MESH)
    pl.semaphore_wait(barrier, len(others))


def rcopy(src, dst, send, recv, to):
    return pltpu.make_async_remote_copy(
        src_ref=src, dst_ref=dst, send_sem=send, recv_sem=recv, device_id=to, device_id_type=MESH
    )


def cuts(weights):
    n = 2 if weights % 256 == 0 else 1
    return [pl.ds(i * (weights // n), weights // n) for i in range(n)]


def depth(chips, k, way):
    return chips // 2 if k == way else chips // 2 - 1


def front_kernel(
    dims, tok, wq, w_out, w_ff1, w_ff2, side0, side1, side2, side3, side4, side5, side6, og, bias, prev, raw, prob, tok_all, proj_all, wf_all, wq_all, vec_all, og_all, att_all,
    tok_s, wq_s, proj_s, q_s, k_s, v_s, att_s, wf, vec, wf_v,
    x_send, x_recv, q_send, q_recv, f_send, f_recv, p_send, p_recv, a_send, a_recv, l_sem,
):
    cols, rows_dev, seqs, heads, pairs, share, block = dims
    at = Spot(rows_dev, cols)
    chips, me, row = at.chips, at.me, at.row
    half_size = cols // 2
    width = heads * DH
    length = prev.shape[2]
    per = length // share
    turns = length // block
    in_share = share // block
    step = pl.program_id(0)
    steps = pairs * seqs * turns
    group = step // turns
    pos = lax.rem(step, turns)
    pair_now = group // seqs
    seq_now = lax.rem(group, seqs)
    turn = lax.rem(pos + lax.rem(me + 1, per) * in_share, turns)
    offs = [j for j in range(1, cols)]
    far = chips // 2
    pieces = cuts(wf.shape[1])
    kinds = ("tok", "tok2", "wf", "vec", "og")
    first = pl.ds(0, tok.shape[0] // 2)
    second = pl.ds(tok.shape[0] // 2, tok.shape[0] // 2)

    def half(k):
        mine = me // half_size
        first = mine if k == 0 else 1 - mine
        return pl.ds(first * half_size, half_size)

    def off(way, h):
        return -h if way == 0 else h

    def q_hop(way, h):
        r = at.row_at(off(way, h - 1))
        src = wq if h == 1 else wq_s.at[r]
        return rcopy(src, wq_s.at[r], q_send.at[way, h - 1], q_recv.at[way, h - 1], at.ring(way))

    def q_got(way, h):
        r = at.row_at(off(way, h))
        return rcopy(wq, wq_s.at[r], q_send.at[way, h - 1], q_recv.at[way, h - 1], at.ring(way))

    def q_pair(way, h, mine=True):
        r = at.row_at(off(way, h))
        src = wq if h == 0 else wq_s.at[r]
        if not mine:
            r = r + 1 - 2 * at.core
        return rcopy(src, wq_s.at[r], q_send.at[2 + way, h], q_recv.at[2 + way, h], at.partner)

    def f_hop(k, p, way, h):
        part = wf_v.at[at.row_at(off(way, h - 1)), half(k), :, pieces[p]]
        return rcopy(part, part, f_send.at[k, p, way, h - 1], f_recv.at[k, p, way, h - 1], at.ring(way))

    def f_got(k, p, way, h):
        part = wf_v.at[at.row_at(off(way, h)), half(k), :, pieces[p]]
        return rcopy(part, part, f_send.at[k, p, way, h - 1], f_recv.at[k, p, way, h - 1], at.ring(way))

    def f_pair(k, p, way, h, mine=True):
        r = at.row_at(off(way, h))
        if not mine:
            r = r + 1 - 2 * at.core
        part = wf_v.at[r, half(k), :, pieces[p]]
        return rcopy(part, part, p_send.at[k, p, way, h], p_recv.at[k, p, way, h], at.partner)

    def f_own(k, p):
        f_hop(k, p, 0, 1).start()
        f_hop(k, p, 1, 1).start()
        f_pair(k, p, 0, 0).start()

    def x_copy(kind, j):
        to = at.peer(j)
        src, dst = {
            "tok": (tok.at[first], tok_s.at[me, first]),
            "tok2": (tok.at[second], tok_s.at[me, second]),
            "wf": (wf, wf_v.at[row, me]),
            "vec": (vec, vec_all.at[me]),
            "og": (og.at[pl.ds(pl.multiple_of(to * share, share), share)], og_all.at[me]),
        }[kind]
        n = kinds.index(kind)
        return rcopy(src, dst, x_send.at[n, j - 1], x_recv.at[n, j - 1], at.col_peer(j))

    def x_got(kind, j):
        came = at.peer(-j)
        src, dst = {
            "tok": (tok.at[first], tok_s.at[came, first]),
            "tok2": (tok.at[second], tok_s.at[came, second]),
            "wf": (wf, wf_v.at[row, came]),
            "vec": (vec, vec_all.at[came]),
            "og": (og.at[pl.ds(0, share)], og_all.at[came]),
        }[kind]
        n = kinds.index(kind)
        return rcopy(src, dst, x_send.at[n, j - 1], x_recv.at[n, j - 1], at.col_peer(j))

    def locals_():
        own = pl.ds(pl.multiple_of(me * share, share), share)
        return [
            pltpu.make_async_copy(wf, wf_v.at[row, me], l_sem.at[0]),
            pltpu.make_async_copy(wq, wq_s.at[row], l_sem.at[1]),
            pltpu.make_async_copy(tok, tok_s.at[me], l_sem.at[2]),
            pltpu.make_async_copy(vec, vec_all.at[me], l_sem.at[3]),
            pltpu.make_async_copy(og.at[own], og_all.at[me], l_sem.at[4]),
        ]

    def saves():
        return [
            pltpu.make_async_copy(tok_s, tok_all, l_sem.at[0]),
            pltpu.make_async_copy(wq_s, wq_all, l_sem.at[1]),
            pltpu.make_async_copy(proj_s, proj_all, l_sem.at[2]),
        ]

    def handle(k, h, only=None):
        for p in range(len(pieces)) if only is None else only:
            for way in range(2):
                if h <= depth(chips, k, way):
                    f_got(k, p, way, h).wait_recv()
                    if h < depth(chips, k, way):
                        f_hop(k, p, way, h + 1).start()
                    f_pair(k, p, way, h).start()

    @pl.when(step == 0)
    def _():
        hw, fw = w_out.shape[1], w_ff1.shape[1]
        wf[:, :hw] = w_out[...]
        wf[:, hw : hw + fw] = w_ff1[...]
        wf[:, hw + fw :] = w_ff2[...]
        feat = vec.shape[1]
        vec[...] = jnp.zeros_like(vec)
        for i, ref in enumerate((side0, side1, side2, side3, side4, side5)):
            vec[i : i + 1, :] = ref[...].reshape(1, feat)
        long = side6[...].reshape(1, fw)
        for i in range(fw // feat):
            vec[6 + i : 7 + i, :] = long[:, i * feat : (i + 1) * feat]
        greet([at.ring(0), at.ring(1), at.partner] + [at.col_peer(j) for j in offs])
        q_hop(0, 1).start()
        q_hop(1, 1).start()
        for kind in ("wf", "tok", "tok2", "vec"):
            for j in offs:
                x_copy(kind, j).start()
        q_pair(0, 0).start()
        for c in locals_():
            c.start()
        for c in locals_():
            c.wait()
        if cols > 2:
            for j in offs:
                x_got("wf", j).wait_recv()
        for h in range(1, far + 1):
            for way in range(2):
                if h <= depth(chips, 0, way):
                    q_got(way, h).wait_recv()
                    if h < depth(chips, 0, way):
                        q_hop(way, h + 1).start()
                    q_pair(way, h).start()
            if h == 1:
                for p in range(len(pieces)):
                    f_own(0, p)
            if h == 3:
                if cols == 2:
                    for j in offs:
                        x_got("wf", j).wait_recv()
                for p in range(len(pieces)):
                    f_own(1, p)
            if h == 3:
                handle(0, 1)
        for j in offs:
            x_copy("og", j).start()
        handle(1, 1)
        for way in range(2):
            for h in range(0 if way == 0 else 1, depth(chips, 0, way) + 1):
                q_pair(way, h, mine=False).wait_recv()
        for j in offs:
            x_got("tok", j).wait_recv()
        rows = wq_s.shape[0] // cols
        chunk = min(512, tok.shape[0])

        def project(i, carry):
            span = pl.ds(pl.multiple_of(i * chunk, chunk), chunk)

            @pl.when(i == tok.shape[0] // chunk // 2)
            def _():
                for j in offs:
                    x_got("tok2", j).wait_recv()

            total = bias[...].reshape(1, -1).astype(F32)
            for c in range(cols):
                w = wq_s[c * rows : (c + 1) * rows].reshape(-1, wq_s.shape[2])
                total = total + dot_nn(tok_s[c, span, :], w)
            proj_s[span, :] = total.astype(BF16)
            return carry

        lax.fori_loop(0, tok.shape[0] // chunk, project, 0)

    @pl.when(pos == 0)
    def _():
        for pair in range(pairs):

            @pl.when(pair_now == pair)
            def _():
                proj = proj_s[pl.ds(pl.multiple_of(seq_now * length, length), length), :]
                q_s[...] = part_of(proj, pair, heads, 0) * jnp.asarray(0.125, BF16)
                k_s[...] = part_of(proj, pair, heads, 1)
                v = part_of(proj, pair, heads, 2)
                for i in range(heads):
                    v_s[i] = pick(v, i, width)

    def att_copy(g, t, to):
        i = lax.rem(me + 1 + t, per)
        j = g // seqs
        return rcopy(
            att_s.at[g, pl.ds(pl.multiple_of(i * share, share), share)],
            att_all.at[me, j],
            a_send.at[g, t],
            a_recv.at[j, me],
            (row, to),
        )

    def att_keep(g, t):
        i = lax.rem(me + 1 + t, per)
        return pltpu.make_async_copy(
            att_s.at[g, pl.ds(pl.multiple_of(i * share, share), share)], att_all.at[me, g // seqs], l_sem.at[3]
        )

    def att_to(g, t):
        return lax.rem(g, seqs) * per + lax.rem(me + 1 + t, per)

    def att_send(done):
        g = done // turns
        t = lax.rem(done, turns) // in_share
        to = att_to(g, t)

        @pl.when(to != me)
        def _():
            att_copy(g, t, to).start()

        @pl.when(to == me)
        def _():
            c = att_keep(g, t)
            c.start()
            c.wait()

    @pl.when((step > 0) & (lax.rem(step, in_share) == 0))
    def _():
        att_send(step - 1)

    at_step = {1: [(0, 2)], 2: [(1, 2)], 4: [(0, 3)], 5: [(1, 3)], 7: [(0, 4), (1, 4)]}
    for h in range(5, far + 1):
        at_step[7] += [(0, h), (1, h)]
    for n, todo in at_step.items():

        @pl.when(step == n * steps // 8)
        def _(todo=todo):
            for k, h in todo:
                handle(k, h)

    @pl.when(step == 1)
    def _():
        for c in saves():
            c.start()

    rows_now = pl.ds(pl.multiple_of(turn * block, block), block)
    raws, probs, out = forward_block(
        q_s[rows_now, :], k_s[...], [v_s[i] for i in range(heads)], [prev[i] for i in range(heads)], width
    )
    for i in range(heads):
        raw[i] = raws[i]
        prob[i] = probs[i]
    att_s[group, rows_now, :] = out.astype(BF16)

    @pl.when(step == steps - 1)
    def _():
        att_send(step)
        for c in saves():
            c.wait()
        for j in offs:
            for kind in kinds:
                x_copy(kind, j).wait_send()
                if kind in ("vec", "og"):
                    x_got(kind, j).wait_recv()
        for way in range(2):
            for h in range(1, depth(chips, 0, way) + 1):
                q_hop(way, h).wait_send()
            for h in range(0 if way == 0 else 1, depth(chips, 0, way) + 1):
                q_pair(way, h).wait_send()
            for k in range(2):
                for p in range(len(pieces)):
                    for h in range(1, depth(chips, k, way) + 1):
                        f_hop(k, p, way, h).wait_send()
                    for h in range(0 if way == 0 else 1, depth(chips, k, way) + 1):
                        f_pair(k, p, way, h).wait_send()
                        f_pair(k, p, way, h, mine=False).wait_recv()
        keep = pltpu.make_async_copy(wf_v, wf_all, l_sem.at[4])
        keep.start()
        for g in range(pairs * seqs):
            for t in range(per):
                to = att_to(g, t)

                @pl.when(to != me)
                def _():
                    att_copy(g, t, to).wait_send()

        for p in range(pairs):
            for j in offs:
                came = at.peer(j)
                rcopy(
                    att_s.at[0, pl.ds(0, share)], att_all.at[came, p], a_send.at[0, 0], a_recv.at[p, came], at.col_peer(j)
                ).wait_recv()
        keep.wait()


def front(cols, rows_dev, seqs, head_count, tok, wq, w_out, w_ff1, w_ff2, sides, og, bias, prev):
    heads = min(2, head_count)
    pairs = head_count // heads
    total, feat = tok.shape
    share = total // cols
    length = prev.shape[-1]
    width = heads * DH
    block = min(256, share)
    turns = length // block
    per = length // share
    in_share = share // block
    chips = rows_dev // 2
    far = chips // 2
    groups = pairs * seqs
    shard = wq.shape[0]
    weights = w_out.shape[1] + 2 * w_ff1.shape[1]
    n = len(cuts(weights))

    def stream(s):
        g = s // turns
        turn = lax.rem(lax.rem(s, turns) + lax.rem(lax.axis_index("col") + 1, per) * in_share, turns)
        return (lax.rem(g, seqs) * pairs + g // seqs, turn, 0)

    def whole(x):
        n = x.ndim
        return pl.BlockSpec(x.shape, lambda s: (0,) * n, pipeline_mode=pl.Buffered(1))

    blocks = pl.BlockSpec((heads, block, length), stream)
    anywhere = pl.BlockSpec(memory_space=pl.ANY)
    dma = pltpu.SemaphoreType.DMA
    shapes = [
        (cols, total, feat),
        (total, wq.shape[1]),
        (rows_dev, cols, shard, weights),
        (rows_dev,) + wq.shape,
        (cols, 16, feat),
        (cols, share, feat),
        (cols, pairs, share, width),
    ]
    return pl.pallas_call(
        functools.partial(front_kernel, (cols, rows_dev, seqs, heads, pairs, share, block)),
        grid=(groups * turns,),
        in_specs=[whole(x) for x in (tok, wq, w_out, w_ff1, w_ff2, *sides, og, bias)] + [blocks],
        out_specs=[blocks, blocks] + [anywhere] * 7,
        out_shape=[jax.ShapeDtypeStruct(prev.shape, BF16)] * 2 + [jax.ShapeDtypeStruct(s, BF16) for s in shapes],
        scratch_shapes=[
            pltpu.VMEM((cols, total, feat), BF16),
            pltpu.VMEM((rows_dev,) + wq.shape, BF16),
            pltpu.VMEM((total, wq.shape[1]), BF16),
            pltpu.VMEM((length, width), BF16),
            pltpu.VMEM((length, width), BF16),
            pltpu.VMEM((heads, length, width), BF16),
            pltpu.VMEM((groups, length, width), BF16),
            pltpu.VMEM((shard, weights), BF16),
            pltpu.VMEM((16, feat), BF16),
            pltpu.VMEM((rows_dev, cols, shard, weights), BF16),
            dma((5, cols - 1)),
            dma((5, cols - 1)),
            dma((4, far + 1)),
            dma((4, far + 1)),
            dma((2, n, 2, far)),
            dma((2, n, 2, far)),
            dma((2, n, 2, far + 1)),
            dma((2, n, 2, far + 1)),
            dma((groups, per)),
            dma((pairs, cols)),
            dma((5,)),
        ],
        compiler_params=pltpu.CompilerParams(
            collective_id=1, has_side_effects=True, vmem_limit_bytes=60 << 20
        ),
        name="front",
    )(tok, wq, w_out, w_ff1, w_ff2, *sides, og, bias, prev)


def back_kernel(
    dims, proj, gvec, wq_in, tok_in, datt, outp, dh, gw, prob, cot,
    pg, out_all, ig, gwo, gqo, gvo,
    datt_s, out_s, dh_s, q_s, k_s, v_s, dq_s, dk_s, dv_s, dp_s,
    own_s, part_s, run_s, run_r, fin_s, fin_r,
    gq_s, gq_p, gq_t, gq_r, ip_s, xi_s, xi_r, vp_s, vs_s, vx_s, vr_s, wq, tok,
    x_send, x_recv, p_send, p_recv, r_send, r_recv, g_send, g_recv, v_send, v_recv, l_sem,
):
    cols, rows_dev, seqs, heads, pairs, share, block = dims
    at = Spot(rows_dev, cols)
    chips, me, core = at.chips, at.me, at.core
    chip = at.row // 2
    half_size = cols // 2
    width = heads * DH
    wide = 3 * width
    length = prob.shape[2]
    per = length // share
    turns = length // block
    in_share = share // block
    shard = gw.shape[3]
    pieces = cuts(gw.shape[4])
    step = pl.program_id(0)
    steps = pairs * seqs * turns
    group = step // turns
    pos = lax.rem(step, turns)
    pair_now = group // seqs
    seq_now = lax.rem(group, seqs)
    turn = lax.rem(pos + lax.rem(me, per) * in_share, turns)
    offs = list(range(1, cols))
    hops = list(range(1, chips))
    far = chips // 2
    total_rows = seqs * length

    def half(k):
        mine = me // half_size
        first = mine if k == 0 else 1 - mine
        return pl.ds(first * half_size, half_size)

    def chip_of(o):
        return chip_at(at.place + o, chips)

    def to_chip(o):
        return (2 * chip_of(o) + core, me)

    halves = [pl.ds(i * (total_rows // 2), total_rows // 2) for i in range(2)]

    def x_copy(kind, j):
        to = at.peer(j)
        src, dst = [
            lambda: (datt.at[to], datt_s.at[me]),
            lambda: (outp.at[to], out_s.at[me]),
            lambda: (dh.at[to], dh_s.at[me]),
            lambda: (fin_s.at[to], fin_r.at[me]),
            lambda: (xi_s.at[j - 1, halves[0]], xi_r.at[j - 1, halves[0]]),
            lambda: (vs_s.at[to], vx_s.at[me]),
            lambda: (xi_s.at[j - 1, halves[1]], xi_r.at[j - 1, halves[1]]),
        ][kind]()
        return rcopy(src, dst, x_send.at[kind, j - 1], x_recv.at[kind, j - 1], at.col_peer(j))

    def x_got(kind, j):
        came = at.peer(-j)
        src, dst = [
            lambda: (datt.at[came], datt_s.at[came]),
            lambda: (outp.at[came], out_s.at[came]),
            lambda: (dh.at[came], dh_s.at[came]),
            lambda: (fin_s.at[came], fin_r.at[came]),
            lambda: (xi_s.at[j - 1, halves[0]], xi_r.at[j - 1, halves[0]]),
            lambda: (vs_s.at[came], vx_s.at[came]),
            lambda: (xi_s.at[j - 1, halves[1]], xi_r.at[j - 1, halves[1]]),
        ][kind]()
        return rcopy(src, dst, x_send.at[kind, j - 1], x_recv.at[kind, j - 1], at.col_peer(j))

    def part_copy(o):
        c = chip_of(o)
        return rcopy(gw.at[c, 1 - core], part_s.at[c], p_send.at[o % chips], p_recv.at[o % chips], at.partner)

    def own_load():
        return pltpu.make_async_copy(gw.at[:, core], own_s, l_sem.at[0])

    def locals_():
        return [
            pltpu.make_async_copy(datt.at[me], datt_s.at[me], l_sem.at[1]),
            pltpu.make_async_copy(outp.at[me], out_s.at[me], l_sem.at[2]),
            pltpu.make_async_copy(dh.at[me], dh_s.at[me], l_sem.at[3]),
        ]

    def late_loads():
        return [
            pltpu.make_async_copy(wq_in, wq, l_sem.at[4]),
            pltpu.make_async_copy(tok_in, tok, l_sem.at[5]),
        ]

    def run_copy(k, p, way, t):
        here = (k, p, way, t - 1)
        return rcopy(run_s.at[here], run_r.at[here], r_send.at[here], r_recv.at[here], at.ring(way))

    waited = set()

    def chip_sum(k, p, o):
        if o % chips not in waited:
            waited.add(o % chips)
            part_copy(o).wait_recv()
        c = chip_of(o)
        return own_s[c, half(k), :, pieces[p]].astype(F32) + part_s[c, half(k), :, pieces[p]].astype(F32)

    def run_step(k, p, t):
        for way in range(2):
            o = depth(chips, k, way) + 1 - t
            if o < 1:
                continue
            value = chip_sum(k, p, o if way == 0 else -o)
            if t > 1:
                run_copy(k, p, way, t - 1).wait_recv()
                value = value + run_r[k, p, way, t - 2].astype(F32)
            run_s[k, p, way, t - 1] = value.astype(BF16)
            run_copy(k, p, way, t).start()

    def run_last(k, p):
        value = chip_sum(k, p, 0)
        for way in range(2):
            d = depth(chips, k, way)
            run_copy(k, p, way, d).wait_recv()
            value = value + run_r[k, p, way, d - 1].astype(F32)
        fin_s[half(k), :, pieces[p]] = value.astype(BF16)

    streams = [(k, p) for p in range(len(pieces)) for k in range(2)]

    def run_round(t, only=None):
        for n, (k, p) in enumerate(streams):
            if only is None or n in only:
                run_step(k, p, t)

    def v_pair():
        return rcopy(gvec, vp_s, v_send.at[0], v_recv.at[0], at.partner)

    def v_chip(o):
        return rcopy(vr_s.at[chip], vr_s.at[chip], v_send.at[o], v_recv.at[o], to_chip(o))

    def v_chip_got(o):
        c = chip_of(-o)
        return rcopy(vr_s.at[c], vr_s.at[c], v_send.at[o], v_recv.at[o], to_chip(o))

    def v_second():
        v_pair().wait_recv()
        vs_s[...] = gvec[...] + vp_s[...]
        for j in offs:
            x_copy(5, j).start()

    def v_third():
        value = vs_s[me]
        for j in offs:
            x_got(5, j).wait_recv()
            value = value + vx_s[at.peer(-j)]
        vr_s[chip] = value
        for o in hops:
            v_chip(o).start()

    def g_pair(j):
        return rcopy(gq_s.at[:, 1 - core], gq_p.at[j], g_send.at[j, 0], g_recv.at[j, 0], at.partner)

    def g_chip(j, o):
        return rcopy(gq_t.at[j, chip_of(o)], gq_r.at[j, chip], g_send.at[j, o], g_recv.at[j, o], to_chip(o))

    def g_chip_got(j, o):
        return rcopy(gq_t.at[j, 0], gq_r.at[j, chip_of(-o)], g_send.at[j, o], g_recv.at[j, o], to_chip(o))

    def g_weight(j):
        slots = chips // cols
        for c in range(cols):
            value = dot_tn(tok[c], dp_s[...]).astype(BF16)
            gq_s[c * slots : (c + 1) * slots, :, :shard, :] = value.reshape(slots, 2, shard, wide)
        sums = col_sum(dp_s[...].astype(F32))
        line = lax.broadcasted_iota(jnp.int32, (16, wide), 0)
        low = jnp.where(line == 0, jnp.broadcast_to(sums, (16, wide)), 0.0).astype(BF16)
        gq_s[:, :, shard:, :] = jnp.broadcast_to(low[None, None], (chips, 2, 16, wide))
        g_pair(j).start()

    def g_pass(j):
        g_pair(j).wait_recv()
        gq_t[j] = (gq_s[:, core].astype(F32) + gq_p[j].astype(F32)).astype(BF16)
        gq_r[j, chip] = gq_t[j, chip]
        for o in hops:
            g_chip(j, o).start()

    def g_last(j):
        for o in hops:
            g_chip_got(j, o).wait_recv()
        value = gq_r[j, 0].astype(F32)
        for c in range(1, chips):
            value = value + gq_r[j, c].astype(F32)
        gqo[:, j * wide : (j + 1) * wide] = value

    chunk = min(512, share)
    parts_of_half = total_rows // 2 // chunk

    def input_part(j, n, part=None):
        slots = rows_dev // cols
        w = wq[pl.ds(at.peer(n) * slots, slots), :, j * wide : (j + 1) * wide].reshape(slots * shard, wide)

        def go(i, carry):
            span = pl.ds(pl.multiple_of(i * chunk, chunk), chunk)
            value = dot_nt(dp_s[span, :], w)
            if j > 0:
                value = value + ip_s[n, span, :]
            if j < pairs - 1:
                ip_s[n, span, :] = value
            elif n > 0:
                xi_s[n - 1, span, :] = value.astype(BF16)
            else:
                ip_s[0, span, :] = value
            return carry

        first = 0 if part is None else part * parts_of_half
        lax.fori_loop(first, 2 * parts_of_half if part is None else first + parts_of_half, go, 0)

    @pl.when(step == 0)
    def _():
        greet(
            [at.ring(0), at.ring(1), at.partner]
            + [at.col_peer(j) for j in offs]
            + [to_chip(o) for o in hops if o not in (1, chips - 1)]
        )
        for j in offs:
            x_copy(0, j).start()
        own_load().start()
        v_pair().start()
        order = [far] + [s * o for o in range(far - 1, 0, -1) for s in (1, -1)] + [0]
        for o in order:
            part_copy(o).start()
        for c in locals_() + late_loads():
            c.start()
        locals_()[0].wait()
        if seqs > 1:
            for j in offs:
                x_got(0, j).wait_recv()

    @pl.when(step == 1)
    def _():
        for c in locals_()[1:] + late_loads():
            c.wait()

    if seqs == 1:

        @pl.when(step == in_share)
        def _():
            for j in offs:
                x_got(0, j).wait_recv()

    @pl.when(pos == 0)
    def _():
        for pair in range(pairs):

            @pl.when(pair_now == pair)
            def _():
                here = proj[pl.ds(pl.multiple_of(seq_now * length, length), length), :]
                q_s[...] = part_of(here, pair, heads, 0) * jnp.asarray(0.125, BF16)
                k = part_of(here, pair, heads, 1)
                for i in range(heads):
                    k_s[i] = pick(k, i, width)
                v_s[...] = part_of(here, pair, heads, 2)

        dk_s[...] = jnp.zeros_like(dk_s)
        dv_s[...] = jnp.zeros_like(dv_s)

    jobs = {
        0: [lambda: own_load().wait(), lambda: run_round(1)],
        1: [v_second, *[lambda kind=kind, j=j: x_copy(kind, j).start() for kind in (1, 2) for j in offs]],
        3: [v_third, lambda: run_round(2, (0,))],
        4: [lambda: run_round(2, (1, 2))],
        5: [lambda: run_round(2, (3,))],
        7: [lambda: run_round(3, (0, 1))],
    }

    def spot(n):
        return (n * steps) // 8

    for n, todo in jobs.items():

        @pl.when(step == spot(n))
        def _(todo=todo):
            for job in todo:
                job()

    @pl.when((step == steps // pairs) & (pairs > 1))
    def _():
        if pairs > 1:
            g_pass(0)

    rows_now = pl.ds(pl.multiple_of(turn * block, block), block)
    q_rows = q_s[rows_now, :]
    source = seq_now * per + turn // in_share
    inside = pl.ds(pl.multiple_of(lax.rem(turn, in_share) * block, block), block)
    dq = dk = dv = None
    for pair in range(pairs):

        @pl.when(pair_now == pair)
        def _():
            dq = dk = dv = None
            d_rows = datt_s[source, inside, pair * width : (pair + 1) * width]
            for i in range(heads):
                d_one = pick(d_rows, i, width)
                d_probs = dot_nt(d_one, v_s[...])
                p = prob[i]
                p_wide = p.astype(F32)
                delta = jnp.sum(d_probs * p_wide, axis=1, keepdims=True)
                low = (p_wide * (d_probs - delta) + cot[i].astype(F32)).astype(BF16)
                pg[i] = low
                a = dot_nn(low, k_s[i])
                b = dot_tn(pick(q_rows, i, width), low)
                c = dot_tn(d_one, p)
                dq = a if dq is None else dq + a
                dk = b if dk is None else dk + b
                dv = c if dv is None else dv + c
            dq_s[rows_now, :] = (dq * 0.125).astype(BF16)
            dk_s[...] += dk
            dv_s[...] += dv

    @pl.when(pos == turns - 1)
    def _():
        parts = [dq_s[...], dk_s[...].T.astype(BF16), dv_s[...].T.astype(BF16)]
        here = pl.ds(pl.multiple_of(seq_now * length, length), length)
        for i in range(heads):
            dp_s[here, i * 3 * DH : (i + 1) * 3 * DH] = jnp.concatenate([p[:, i * DH : (i + 1) * DH] for p in parts], axis=1)

    for j in range(pairs - 1):

        @pl.when(step == (j + 1) * (steps // pairs) - 1)
        def _():
            g_weight(j)
            for n in range(cols):
                input_part(j, n)

    @pl.when(step == steps - 1)
    def _():
        last = pairs - 1
        for part, kind in ((0, 4), (1, 6)):
            for j in offs:
                input_part(last, j, part)
                x_copy(kind, j).start()
        if pairs > 1:
            g_pair(last - 1).wait_send()
        run_round(3, (2, 3))
        run_round(4)
        g_weight(last)
        for t in range(5, far + 1):
            run_round(t)
        input_part(last, 0)
        g_pass(last)
        for j in offs:
            x_got(1, j).wait_recv()
            x_got(2, j).wait_recv()
        keep = pltpu.make_async_copy(out_s, out_all, l_sem.at[1])
        keep.start()
        for k, p in streams:
            run_last(k, p)
        for j in offs:
            x_copy(3, j).start()
        for o in hops:
            v_chip_got(o).wait_recv()
        value = vr_s[0]
        for c in range(1, chips):
            value = value + vr_s[c]
        gvo[...] = value
        for j in range(pairs):
            g_last(j)

        def finish(i, carry):
            rows = chunk
            c = i // (share // rows)
            inner = pl.ds(pl.multiple_of(lax.rem(i, share // rows) * rows, rows), rows)
            span = pl.ds(pl.multiple_of(i * rows, rows), rows)
            value = ip_s[0, span, :] + dh_s[c, inner, :].astype(F32)
            for j in offs:
                value = value + xi_r[j - 1, span, :].astype(F32)
            ig[span, :] = value.astype(BF16)
            return carry

        for part, kind in ((0, 4), (1, 6)):
            for j in offs:
                x_got(kind, j).wait_recv()
            lax.fori_loop(part * parts_of_half, (part + 1) * parts_of_half, finish, 0)
        value = fin_s[me].astype(F32)
        for j in offs:
            x_got(3, j).wait_recv()
            value = value + fin_r[at.peer(-j)].astype(F32)
        gwo[...] = value
        keep.wait()
        for kind in range(7):
            for j in offs:
                x_copy(kind, j).wait_send()
        for o in range(chips):
            part_copy(o).wait_send()
        for k in range(2):
            for way in range(2):
                for t in range(1, depth(chips, k, way) + 1):
                    for p in range(len(pieces)):
                        run_copy(k, p, way, t).wait_send()
        v_pair().wait_send()
        for o in hops:
            v_chip(o).wait_send()
        g_pair(last).wait_send()
        for j in range(pairs):
            for o in hops:
                g_chip(j, o).wait_send()


def back(cols, rows_dev, seqs, head_count, proj, wq, tok, datt, outp, dh, gvec, gw, prob, cot):
    heads = min(2, head_count)
    pairs = head_count // heads
    _, total, feat = tok.shape
    share = total // cols
    length = prob.shape[-1]
    width = heads * DH
    wide = 3 * width
    block = min(256, share)
    turns = length // block
    per = length // share
    in_share = share // block
    chips = rows_dev // 2
    far = chips // 2
    shard, weights = gw.shape[2:]
    half_size = cols // 2
    n = len(cuts(weights))
    gw = gw.reshape(chips, 2, cols, shard, weights)

    def stream(s):
        g = s // turns
        turn = lax.rem(lax.rem(s, turns) + lax.rem(lax.axis_index("col"), per) * in_share, turns)
        return (lax.rem(g, seqs) * pairs + g // seqs, turn, 0)

    def whole(shape):
        n = len(shape)
        return pl.BlockSpec(shape, lambda s: (0,) * n, pipeline_mode=pl.Buffered(1))

    blocks = pl.BlockSpec((heads, block, length), stream)
    anywhere = pl.BlockSpec(memory_space=pl.ANY)
    dma = pltpu.SemaphoreType.DMA
    outs = [
        jax.ShapeDtypeStruct(prob.shape, BF16),
        jax.ShapeDtypeStruct((cols, share, feat), BF16),
        jax.ShapeDtypeStruct((total, feat), BF16),
        jax.ShapeDtypeStruct((shard, weights), F32),
        jax.ShapeDtypeStruct((shard + 16, wq.shape[2]), F32),
        jax.ShapeDtypeStruct(gvec.shape[1:], F32),
    ]
    return pl.pallas_call(
        functools.partial(back_kernel, (cols, rows_dev, seqs, heads, pairs, share, block)),
        grid=(pairs * seqs * turns,),
        in_specs=[whole(proj.shape), whole(gvec.shape)] + [anywhere] * 6 + [blocks, blocks],
        out_specs=[blocks, anywhere] + [whole(o.shape) for o in outs[2:]],
        out_shape=outs,
        scratch_shapes=[
            pltpu.VMEM(datt.shape, BF16),
            pltpu.VMEM(outp.shape, BF16),
            pltpu.VMEM(dh.shape, BF16),
            pltpu.VMEM((length, width), BF16),
            pltpu.VMEM((heads, length, width), BF16),
            pltpu.VMEM((length, width), BF16),
            pltpu.VMEM((length, width), BF16),
            pltpu.VMEM((width, length), F32),
            pltpu.VMEM((width, length), F32),
            pltpu.VMEM((total, wide), BF16),
            pltpu.VMEM((chips, cols, shard, weights), BF16),
            pltpu.VMEM((chips, cols, shard, weights), BF16),
            pltpu.VMEM((2, n, 2, far, half_size, shard, weights // n), BF16),
            pltpu.VMEM((2, n, 2, far, half_size, shard, weights // n), BF16),
            pltpu.VMEM((cols, shard, weights), BF16),
            pltpu.VMEM((cols, shard, weights), BF16),
            pltpu.VMEM((chips, 2, shard + 16, wide), BF16),
            pltpu.VMEM((pairs, chips, shard + 16, wide), BF16),
            pltpu.VMEM((pairs, chips, shard + 16, wide), BF16),
            pltpu.VMEM((pairs, chips, shard + 16, wide), BF16),
            pltpu.VMEM((cols if pairs > 1 else 1, total, feat), F32),
            pltpu.VMEM((cols - 1, total, feat), BF16),
            pltpu.VMEM((cols - 1, total, feat), BF16),
            pltpu.VMEM(gvec.shape, F32),
            pltpu.VMEM(gvec.shape, F32),
            pltpu.VMEM(gvec.shape, F32),
            pltpu.VMEM((chips,) + gvec.shape[1:], F32),
            pltpu.VMEM(wq.shape, BF16),
            pltpu.VMEM(tok.shape, BF16),
            dma((7, cols - 1)),
            dma((7, cols - 1)),
            dma((chips,)),
            dma((chips,)),
            dma((2, n, 2, far)),
            dma((2, n, 2, far)),
            dma((pairs, chips)),
            dma((pairs, chips)),
            dma((chips,)),
            dma((chips,)),
            dma((6,)),
        ],
        compiler_params=pltpu.CompilerParams(
            collective_id=2, has_side_effects=True, vmem_limit_bytes=62 << 20
        ),
        name="back",
    )(proj, gvec, wq, tok, datt, outp, dh, gw, prob, cot)


def finish_kernel(
    pg_in, out_in, ig_in, gw, gq, gv, pg, out, ig, wq, bq, wo, bo, n1g, n1s, w1, b1, w2, b2, n2g, n2s,
    bounce, out_s, ig_s, in_sem, out_sem,
):
    ways = [(pg_in.at[n], bounce.at[n], pg.at[n]) for n in range(bounce.shape[0])]
    ways += [(out_in, out_s, out), (ig_in, ig_s, ig)]
    slots = len(ways)
    takes = [pltpu.make_async_copy(a, b, in_sem.at[n]) for n, (a, b, _) in enumerate(ways)]
    puts = [pltpu.make_async_copy(b, c, out_sem.at[n]) for n, (_, b, c) in enumerate(ways)]
    for c in takes:
        c.start()
    shard = wq.shape[0]
    hw, fw = wo.shape[1], w1.shape[1]
    feat = gv.shape[1]
    for n in range(slots // 2):
        takes[n].wait()
        puts[n].start()
    wq[...] = gq[:shard]
    bq[...] = gq[shard : shard + 1].reshape(-1)
    wo[...] = gw[:, :hw]
    w1[...] = gw[:, hw : hw + fw]
    w2[...] = gw[:, hw + fw :]
    for i, ref in enumerate((bo, n1g, n1s, b2, n2g, n2s)):
        ref[...] = gv[i : i + 1].reshape(-1)
    b1[...] = jnp.concatenate([gv[6 + i : 7 + i] for i in range(fw // feat)], axis=1).reshape(-1)
    for n in range(slots // 2, slots):
        takes[n].wait()
        puts[n].start()
    for c in puts:
        c.wait()


def finish(pg, out, ig, gw, gq, gv, hw, fw):
    slots = 4
    pieces = (slots, pg.shape[0] * pg.shape[1] // slots, pg.shape[2])
    total, feat = ig.shape
    shard = gw.shape[0]
    vmem = pl.BlockSpec(memory_space=pltpu.VMEM)
    anywhere = pl.BlockSpec(memory_space=pl.ANY)

    def f32(*shape):
        return jax.ShapeDtypeStruct(shape, F32)

    outs = [
        jax.ShapeDtypeStruct(pieces, BF16),
        jax.ShapeDtypeStruct(ig.shape, BF16),
        jax.ShapeDtypeStruct(ig.shape, BF16),
        f32(shard, gq.shape[1]),
        f32(gq.shape[1]),
        f32(shard, hw),
        f32(feat),
        f32(feat),
        f32(feat),
        f32(shard, fw),
        f32(fw),
        f32(shard, fw),
        f32(feat),
        f32(feat),
        f32(feat),
    ]
    return pl.pallas_call(
        finish_kernel,
        out_shape=outs,
        in_specs=[anywhere] * 3 + [vmem] * 3,
        out_specs=[anywhere] * 3 + [vmem] * 12,
        scratch_shapes=[
            pltpu.VMEM(pieces, BF16),
            pltpu.VMEM(ig.shape, BF16),
            pltpu.VMEM(ig.shape, BF16),
            pltpu.SemaphoreType.DMA((slots + 2,)),
            pltpu.SemaphoreType.DMA((slots + 2,)),
        ],
        compiler_params=pltpu.CompilerParams(vmem_limit_bytes=60 << 20),
        name="finish",
    )(pg.reshape(pieces), out.reshape(ig.shape), ig, gw, gq, gv)


def per_device(
    cols,
    row_count,
    tokens,
    prev_logits,
    qkv_weight,
    qkv_bias,
    out_weight,
    out_bias,
    norm1_gain,
    norm1_shift,
    ff1_weight,
    ff1_bias,
    ff2_weight,
    ff2_bias,
    norm2_gain,
    norm2_shift,
    out_grad,
    logit_grad,
):
    seqs, head_count, length, _ = prev_logits.shape
    total, feat = tokens.shape
    share = total // cols
    rows = min(256, length)
    rows_dev = row_count
    hidden = ff1_weight.shape[1]
    sides = (out_bias, norm1_gain, norm1_shift, ff2_bias, norm2_gain, norm2_shift, ff1_bias)
    prev = prev_logits.reshape(seqs * head_count, length, length)
    cot = logit_grad.reshape(seqs * head_count, length, length)
    raw, prob, tok_all, proj, wf_all, wq_all, vec_all, og_all, att_all = front(
        cols, rows_dev, seqs, head_count, tokens, qkv_weight, out_weight.T, ff1_weight, ff2_weight.T, sides, out_grad, qkv_bias, prev
    )
    out, dh, datt, gvec, gw, raw = middle(tok_all, att_all, og_all, wf_all, vec_all, raw)

    prev_grad, output, input_grad, gw, gq, gv = back(
        cols, rows_dev, seqs, head_count, proj, wq_all, tok_all, datt, out, dh, gvec, gw, prob, cot
    )
    prev_grad, output, input_grad, *rest = finish(
        prev_grad, output, input_grad, gw, gq, gv, out_weight.shape[0], hidden
    )
    rest[2] = rest[2].T
    rest[8] = rest[8].T
    return output, raw.reshape(prev_logits.shape), input_grad, prev_grad.reshape(prev_logits.shape), *rest


def solution(mesh):
    in_specs = (
        P("row", "col"),
        P("row", "col", None, None),
        P("row", "col"),
        P("col"),
        P("col", "row"),
        P("col"),
        P("col"),
        P("col"),
        P("row", "col"),
        P("col"),
        P("col", "row"),
        P("col"),
        P("col"),
        P("col"),
        P("row", "col"),
        P("row", "col", None, None),
    )
    out_specs = (
        P("row", "col"),
        P("row", "col", None, None),
        P("row", "col"),
        P("row", "col", None, None),
        P("row", "col"),
        P("col"),
        P("col", "row"),
        P("col"),
        P("col"),
        P("col"),
        P("row", "col"),
        P("col"),
        P("col", "row"),
        P("col"),
        P("col"),
        P("col"),
    )
    return jax.shard_map(
        functools.partial(per_device, mesh.shape["col"], mesh.shape["row"]),
        mesh=mesh,
        in_specs=in_specs,
        out_specs=out_specs,
        check_vma=False,
    )
```
